32 devices in a mesh: seq: 2 (over core), vocab: 16 (over z, y, x).
Axes of the slice: x: 2, y: 2, z: 4, core: 2. Of those that a mesh axis runs over, the one named last changes fastest.
Arguments:
- hidden: bfloat16 [1024, 8192], P('seq', 'vocab'), may hold values from -80 to 80
- weight: bfloat16 [8192, 8192], P('seq', 'vocab'), may hold values from -0.06629126 to 0.06629126, as said below
- tangent: bfloat16 [8192, 8192], P('seq', 'vocab'), may hold values from -0.0625 to 0.0625
- targets: int32 [1024], P('seq'), may hold values from 0 to 8191
Outputs:
- ggn: bfloat16 [8192, 8192], P('seq', 'vocab')
- token_loss: float32 [1024], P('seq')
The draws below stay inside these ranges and needn't reach their ends.
Inputs may be any that keep to these rules, and one draw needn't show every extreme that they name: `weight`: entries of standard deviation about 8192 ** -0.5.
All inputs are finite; a program needn't handle non-finite values.
Results may differ from the reference program's by a relative error of at most 0.0065.
Values may be sent and summed in bfloat16 or wider, within the bound.
A program may use at most 64 MiB of HBM per device.

```python
import math
import jax
import jax.numpy as jnp
from jax import lax

D = 8192
V_DEV = 512
VOCAB = 8192
TOKENS = 1024
N_VOCAB = 16


def joint_weight(key):
    limit = 6.0 / math.sqrt(D)
    raw = jax.random.normal(jax.random.fold_in(key, 101), (D, VOCAB), jnp.float32) / math.sqrt(D)
    return jnp.clip(raw, -limit, limit)


def draw_weight(key, part):
    return joint_weight(key).astype(jnp.bfloat16)


def draw_hidden(key, part):
    hidden_key = jax.random.fold_in(key, 202)
    normal_part = 3.0 * jax.random.normal(hidden_key, (TOKENS, D), jnp.float32)
    return normal_part.astype(jnp.bfloat16)


def set_ends(result, stream_key, low, top_value):
    longest = result.shape.index(max(result.shape))
    spots = []
    for shift in (0, 1):
        where = [jax.random.randint(jax.random.fold_in(stream_key, axis), (), 0, length) for axis, length in enumerate(result.shape)]
        where[longest] = (where[longest] + shift) % result.shape[longest]
        spots.append(tuple(where))
    return result.at[spots[0]].set(low).at[spots[1]].set(top_value)


def shard_levels(stream_key, dims, cuts, smallest, high):
    gain, own = 1.0, jax.random.fold_in(stream_key, 6)
    for axis_at, blocks in cuts:
        steps = jnp.exp(jax.random.uniform(jax.random.fold_in(own, axis_at), (blocks,), jnp.float32, smallest / len(cuts), high / len(cuts)))
        gain = gain * jnp.repeat(steps, dims[axis_at] // blocks).reshape([-1 if axis == axis_at else 1 for axis in range(len(dims))])
    return gain


def normal_values(stream_key, dims, deviation, most, split=(), held_as=jnp.bfloat16):
    values = jax.random.normal(stream_key, dims, jnp.float32) * deviation
    if len(split) > 0:
        values = shard_levels(stream_key, dims, split, -0.22, 0.18) * values
    return jnp.clip(values, min=-most, max=most).astype(held_as)


def setup_inputs(seed: int = 0) -> dict:
    splits = jax.random.split(jax.random.key(seed), 5)
    hidden = draw_hidden(jax.random.fold_in(splits[4], 71), 0)
    weight = draw_weight(jax.random.fold_in(splits[4], 71), 0)
    tangent = normal_values(splits[2], (D, VOCAB), D ** -0.5, 0.0625, ((0, 2), (1, 16)))
    targets = set_ends(jax.random.randint(splits[3], (TOKENS,), 0, VOCAB), jax.random.fold_in(splits[3], 1), 0, VOCAB - 1).astype(jnp.int32)
    return dict(hidden=hidden, weight=weight, tangent=tangent, targets=targets)


def reference(hidden, weight, tangent, targets):
    logits = jnp.dot(hidden, weight, preferred_element_type=jnp.float32)
    tangent_logits = jnp.dot(hidden, tangent, preferred_element_type=jnp.float32)
    row_top = jnp.max(logits, axis=1, keepdims=True)
    exp_logits = jnp.exp(logits - row_top)
    totals = jnp.sum(exp_logits, axis=1, keepdims=True)
    expect = jnp.sum(exp_logits * tangent_logits, axis=1, keepdims=True) / totals
    columns = jnp.arange(VOCAB, dtype=jnp.int32)
    picked = jnp.sum(jnp.where(columns[None, :] == targets[:, None], logits, jnp.float32(0.0)), axis=1)
    token_loss = row_top[:, 0] + jnp.log(totals[:, 0]) - picked
    weight_term = (exp_logits / totals * (tangent_logits - expect)).astype(jnp.bfloat16)
    blocked = weight_term.reshape(TOKENS, N_VOCAB, V_DEV).transpose(1, 0, 2)

    def one_block(term_block):
        return jnp.einsum("td,tv->dv", hidden.astype(jnp.float32), term_block.astype(jnp.float32)).astype(jnp.bfloat16)

    pieces = lax.map(one_block, blocked)
    ggn = pieces.transpose(1, 0, 2).reshape(D, VOCAB)
    return ggn, token_loss
```

```python
import functools

import jax
import jax.numpy as jnp
from jax import lax
from jax.experimental import pallas as pl
from jax.experimental.pallas import tpu as pltpu
from jax.sharding import PartitionSpec as P

MESH = pl.DeviceIdType.MESH
PLANE, DEPTH = 4, 4
CHUNKS = 8
GROUPS = CHUNKS // 2
LEAD = 3
LAGS = ((0, 0, 2, 2, 2, 2, 4, 4), (0, 0, 2, 2, 2, 2, 4, 4), (0, 0, 2, 2, 2, 2, 4, 4), (0, 0, 2, 2, 2, 2, 4, 4))
ORDERS = ((0, 1, 2, 3, 4, 5, 6, 7), (0, 1, 2, 3, 4, 5, 6, 7), (0, 1, 2, 3, 4, 5, 6, 7), (0, 1, 2, 3, 4, 5, 6, 7))
TALL = (0, 0, 0, 255, 0, 0, 0, 0)
DEEP = (0, 0, 0, 15, 0, 0, 0, 0)
VIA = (0, 255, 0, 255, 255, 0, 255, 0)
LANES = 128


def links_used(zz, y, x):
    used = [0, 0, 0, 0]
    for c in range(CHUNKS):
        for item in range(8):
            szz, dy, dx = item // 4, item // 2 % 2, item % 2
            spot = (y + dy) % 2 * 2 + (x + dx) % 2
            tall = TALL[c] >> (szz * 4 + spot) & 1
            deep = DEEP[c] >> spot & 1 and szz == 1
            via = VIA[c] >> (szz * 4 + spot) & 1
            column = dx + dy == 0
            inplane = not (zz > szz and tall or zz < szz and deep)
            used[0] += inplane and (column or (dx == 0 and dy == 1 and via == 1))
            used[1] += inplane and (column or (dx == 1 and dy == 0 and via == 0))
            used[2] += (column or tall) and zz >= szz and zz < DEPTH - 1
            used[3] += (column or deep) and zz == 1 and szz == 1
    return [int(u) for u in used]


def packed(values, bits):
    word = sum(value << (bits * i) for i, value in enumerate(values))
    return word - (word >> 31 << 32)


def pick(index, values):
    chosen = jnp.int32(values[0])
    for i, value in enumerate(values[1:]):
        chosen = jnp.where(index == i + 1, jnp.int32(value), chosen)
    return chosen


def field(word, index, bits):
    return (word >> (index * bits)) & (2**bits - 1)


def gather_kernel(
    n, hidden, weight, tangent, targets, total, last, term, loss_out,
    hid, flipped, staged, wv, tv, part, far, stats, target, target_pair, wanted,
    recv, sent, pair_recv, pair_sent, load_sem, far_sent, far_recv,
    stat_sent, stat_recv, target_sem, hello,
):
    s = lax.axis_index("seq")
    v = lax.axis_index("vocab")
    half_n = n // 2
    rows = hid.shape[1]
    half = rows // 2
    group_rows = 2 * rows
    width = wv.shape[2]
    z, y, x = v // PLANE, (v // 2) % 2, v % 2
    zz = z + s * (DEPTH - 1 - 2 * z)
    up_step = PLANE * (1 - 2 * s)
    x_dev = (s, v + 1 - 2 * x)
    y_dev = (s, v + 2 - 4 * y)
    up_dev = (s, v + up_step)
    down_dev = (s, v - up_step)
    pair_dev = (1 - s, v)
    is_source = zz < DEPTH // 2
    has_up = zz < DEPTH - 1
    has_down = zz > 0
    along_count = has_up.astype(jnp.int32) + has_down.astype(jnp.int32)
    own_k = jnp.where(is_source, v - half_n * s, 0)
    pair_k = jnp.where(is_source, 0, v - half_n * (1 - s))
    lag_word = pick(zz, [packed(lags, 4) for lags in LAGS])
    order_word = pick(zz, [packed(order, 3) for order in ORDERS])
    last_lag = pick(zz, [max(lags) for lags in LAGS])
    finish_lag = jnp.where(is_source, 4, 2)

    mine = pl.ds(pl.multiple_of(s * half, half), half)
    theirs = pl.ds(pl.multiple_of((1 - s) * half, half), half)

    load_w = pltpu.make_async_copy(weight, wv, load_sem.at[0])
    load_t = pltpu.make_async_copy(tangent, tv, load_sem.at[1])
    load_target = pltpu.make_async_copy(targets, target, load_sem.at[2])

    own_load = pltpu.make_async_copy(hidden, hid.at[pl.ds(own_k * CHUNKS, CHUNKS), mine], load_sem.at[3])
    stage = pltpu.make_async_copy(hidden, staged, load_sem.at[3])

    def pair_copy(k, c, span):
        return pltpu.make_async_remote_copy(
            src_ref=staged.at[c],
            dst_ref=hid.at[k * CHUNKS + c, span],
            send_sem=pair_sent.at[0],
            recv_sem=pair_recv.at[c],
            device_id=pair_dev,
            device_id_type=MESH,
        )

    def bulk(ref, semaphore):
        return pltpu.make_async_remote_copy(
            src_ref=ref,
            dst_ref=ref,
            send_sem=semaphore,
            recv_sem=semaphore,
            device_id=pair_dev,
            device_id_type=MESH,
        )

    def greet(semaphore, device):
        pl.semaphore_signal(semaphore, inc=1, device_id=device, device_id_type=MESH)

    def greet_along(semaphore):
        @pl.when(has_up)
        def _():
            greet(semaphore, up_dev)

        @pl.when(has_down)
        def _():
            greet(semaphore, down_dev)

    barrier = pltpu.get_barrier_semaphore()
    greet(barrier, pair_dev)
    greet(barrier, x_dev)
    greet(barrier, y_dev)
    greet_along(barrier)

    @pl.when(is_source)
    def _():
        own_load.start()

    @pl.when(jnp.logical_not(is_source))
    def _():
        stage.start()

    load_target.start()
    load_w.start()
    load_t.start()

    def clear(i, carry):
        part[i] = jnp.zeros(part.shape[1:], jnp.float32)
        total[i] = jnp.zeros(total.shape[1:], jnp.float32)
        return carry

    lax.fori_loop(0, CHUNKS, clear, 0)
    loss_out[...] = jnp.zeros_like(loss_out)
    load_target.wait()
    pl.semaphore_wait(barrier, 3 + along_count)
    greet(hello.at[0], x_dev)
    pair_target = pltpu.make_async_remote_copy(
        src_ref=target,
        dst_ref=target_pair,
        send_sem=target_sem.at[0],
        recv_sem=target_sem.at[1],
        device_id=pair_dev,
        device_id_type=MESH,
    )
    pair_target.start()

    @pl.when(jnp.logical_not(is_source))
    def _():
        stage.wait()

        def give(c, carry):
            pair_copy(pair_k, c, mine).start()
            return carry

        lax.fori_loop(0, CHUNKS, give, 0)

    @pl.when(is_source)
    def _():
        own_load.wait()

    def copy(link, k, c, device, span):
        piece = hid.at[k * CHUNKS + c, span]
        return pltpu.make_async_remote_copy(
            src_ref=piece,
            dst_ref=piece,
            send_sem=sent.at[link],
            recv_sem=recv.at[k, c],
            device_id=device,
            device_id_type=MESH,
        )

    def routes(k, c, dx, dy, szz, span):
        column = dx + dy == 0
        spot = ((y + dy) % 2) * 2 + (x + dx) % 2
        word = pick(c, [TALL[i] | VIA[i] << 8 | DEEP[i] << 20 for i in range(CHUNKS)])
        place = szz * 4 + spot
        tall = field(word, place, 1) == 1
        via = field(word, place + 8, 1)
        deep = field(word, place + 16, 1) == 1
        along = jnp.logical_or(
            jnp.logical_and(zz > szz, tall), jnp.logical_and(zz < szz, deep)
        )
        inplane = jnp.logical_not(along)
        via_x = jnp.logical_and(jnp.logical_and(dx == 0, dy == 1), via == 1)
        via_y = jnp.logical_and(jnp.logical_and(dx == 1, dy == 0), via == 0)
        go_up = jnp.logical_and(jnp.logical_or(column, tall), jnp.logical_and(zz >= szz, has_up))
        go_down = jnp.logical_and(jnp.logical_or(column, deep), jnp.logical_and(zz == 1, szz == 1))
        return (
            (go_up, copy(2, k, c, up_dev, span)),
            (go_down, copy(3, k, c, down_dev, span)),
            (jnp.logical_and(inplane, jnp.logical_or(column, via_x)), copy(0, k, c, x_dev, span)),
            (jnp.logical_and(inplane, jnp.logical_or(column, via_y)), copy(1, k, c, y_dev, span)),
        )

    def forward(k, c, dx, dy, szz, span):
        for condition, route in routes(k, c, dx, dy, szz, span):
            @pl.when(condition)
            def _():
                route.start()

    everything = pl.ds(0, rows)

    def item(q):
        r, i = q // 2, q % 2
        dx, dy = r % 2, r // 2
        first = jnp.where(zz >= 1, 1, 0)
        szz = first + i * (1 - 2 * first)
        src_z = szz + s * (DEPTH - 1 - 2 * szz)
        k = src_z * PLANE + ((y + dy) % 2) * 2 + (x + dx) % 2 - half_n * s
        return k, dx, dy, szz

    def send_own(c):
        @pl.when(jnp.logical_and(is_source, c < CHUNKS))
        def _():
            forward(own_k, c, 0, 0, zz, mine)
            pair_copy(own_k, c, theirs).wait_recv()
            forward(own_k, c, 0, 0, zz, theirs)

    def lead(c, carry):
        send_own(c)
        return carry

    lax.fori_loop(0, LEAD, lead, 0)
    load_w.wait()
    load_t.wait()

    def far_copy(c):
        return pltpu.make_async_remote_copy(
            src_ref=part.at[c],
            dst_ref=far.at[c],
            send_sem=far_sent.at[0],
            recv_sem=far_recv.at[c],
            device_id=pair_dev,
            device_id_type=MESH,
        )

    def stat_copy(c, core, d):
        return pltpu.make_async_remote_copy(
            src_ref=stats.at[c, 0],
            dst_ref=stats.at[c, d],
            send_sem=stat_sent.at[core],
            recv_sem=stat_recv.at[c],
            device_id=(core, (v + d) % n),
            device_id_type=MESH,
        )

    def local_stats(c):
        far_copy(c).wait_recv()

        both = part[c] + far[c]
        logits, slope = both[:, :width], both[:, width:]
        top = jnp.max(logits, axis=1, keepdims=True)
        e = jnp.exp(logits - top)
        amount = jnp.sum(e, axis=1, keepdims=True)
        weighted = jnp.sum(e * slope, axis=1, keepdims=True)
        columns = lax.broadcasted_iota(jnp.int32, logits.shape, 1) + v * width
        picked = jnp.sum(jnp.where(columns == wanted[c][:, 0:1], logits, 0.0), axis=1, keepdims=True)
        lane = lax.broadcasted_iota(jnp.int32, (rows, LANES), 1)
        packed = jnp.where(lane == 0, top, jnp.where(lane == 1, amount, jnp.where(lane == 2, weighted, picked)))
        stats[c, 0] = packed.T[:4]

        stat_copy(c, 1 - s, 0).start()

        def start(d, carry):
            stat_copy(c, 0, n - d).start()
            stat_copy(c, 1, n - d).start()
            return carry

        lax.fori_loop(1, n, start, 0)

    def finish(c):
        @pl.when(is_source)
        def _():
            far_copy(c).wait_recv()
            bulk(stats.at[c], stat_recv.at[c]).wait_recv()

        @pl.when(jnp.logical_not(is_source))
        def _():
            bulk(stats.at[c, pl.ds(1, n - 1)], stat_recv.at[c]).wait_recv()

        every = stats[c]
        tops = every[:, 0, :]
        row_top = jnp.max(tops, axis=0, keepdims=True)
        scale = jnp.exp(tops - row_top)
        totals = jnp.sum(scale * every[:, 1, :], axis=0, keepdims=True)
        tangent_sum = jnp.sum(scale * every[:, 2, :], axis=0, keepdims=True)
        picked = jnp.sum(every[:, 3, :], axis=0, keepdims=True)
        expect = tangent_sum / totals
        line = lax.broadcasted_iota(jnp.int32, (LANES, rows), 0)
        side = jnp.where(line == 0, row_top, jnp.where(line == 1, totals, expect)).T
        both = part[c] + far[c]
        value = jnp.exp(both[:, :width] - side[:, 0:1]) / side[:, 1:2] * (both[:, width:] - side[:, 2:3])
        term[c] = value.astype(term.dtype)
        loss = row_top + jnp.log(totals) - picked
        place = c % 2
        loss = jnp.where(place == s, loss, pltpu.roll(loss, half, 1))
        lane = lax.broadcasted_iota(jnp.int32, (1, rows), 1)
        kept = loss_out[c // 2]
        loss_out[c // 2] = jnp.where(lane // half == place, loss, kept)

    def product(g, k):
        left = flipped[k, :, pl.ds(pl.multiple_of(g * group_rows, group_rows), group_rows)]
        right = term[pl.ds(2 * g, 2)].reshape(group_rows, width)
        total[k] += jnp.dot(left, right, preferred_element_type=jnp.float32)

    def product_due(done):
        late = done - finish_lag - 2
        return jnp.logical_and(late >= 0, jnp.logical_and(late % 2 == 0, late < CHUNKS - 2)), late // 2

    def stages(done):
        @pl.when(jnp.logical_and(jnp.logical_not(is_source), jnp.logical_and(done >= 0, done < CHUNKS)))
        def _():
            local_stats(done)

        @pl.when(done >= finish_lag)
        def _():
            finish(done - finish_lag)

    def step(t, carry):
        done = t - last_lag

        @pl.when(t == 0)
        def _():
            pl.semaphore_wait(hello.at[0], 1)
            greet(hello.at[1], y_dev)

        @pl.when(t == 1)
        def _():
            pl.semaphore_wait(hello.at[1], 1)
            greet_along(hello.at[2])

        @pl.when(t == 2)
        def _():
            pair_target.wait()
            for g in range(GROUPS):
                for ids, side in ((target, mine), (target_pair, theirs)):
                    upright = jnp.broadcast_to(ids[:, g * rows : (g + 1) * rows], (LANES, rows)).T
                    wanted[2 * g, side, :] = upright[:half]
                    wanted[2 * g + 1, side, :] = upright[half:]

            pl.semaphore_wait(hello.at[2], along_count)
            greet_along(hello.at[3])

        @pl.when(t == 3)
        def _():
            pl.semaphore_wait(hello.at[3], along_count)
            greet_along(hello.at[4])

        send_own(t + LEAD)
        ready, g_ready = product_due(done)

        def one(i, inner):
            q = field(order_word, i, 3)
            c = t - field(lag_word, q, 4)

            @pl.when(jnp.logical_and(c >= 0, c < CHUNKS))
            def _():
                k, dx, dy, szz = item(q)
                own = jnp.logical_and(dx + dy == 0, szz == zz)

                @pl.when(jnp.logical_not(own))
                def _():
                    copy(0, k, c, x_dev, everything).wait_recv()
                    forward(k, c, dx, dy, szz, everything)

                piece = hid[k * CHUNKS + c]
                part[c, :, :width] += jnp.dot(piece, wv[k], preferred_element_type=jnp.float32)
                part[c, :, width:] += jnp.dot(piece, tv[k], preferred_element_type=jnp.float32)

                @pl.when(c < CHUNKS - 2)
                def _():
                    flipped[k, :, pl.ds(pl.multiple_of(c * rows, rows), rows)] = hid[k * CHUNKS + c].T

                @pl.when(c >= CHUNKS - 2)
                def _():
                    at = (c - CHUNKS + 2) * rows
                    last[k, :, pl.ds(pl.multiple_of(at, rows), rows)] = hid[k * CHUNKS + c].T

            @pl.when(ready)
            def _():
                product(g_ready, i)

            return inner

        lax.fori_loop(0, 8, one, 0)

        @pl.when(done == 0)
        def _():
            pl.semaphore_wait(hello.at[4], along_count)

        @pl.when(done >= 0)
        def _():
            far_copy(done).start()

        stages(done)
        return carry

    lax.fori_loop(0, CHUNKS + last_lag, step, 0)

    def after(done, carry):
        stages(done)
        ready, g_ready = product_due(done)

        @pl.when(ready)
        def _():
            def one(k, inner):
                product(g_ready, k)
                return inner

            lax.fori_loop(0, half_n, one, 0)

        return carry

    lax.fori_loop(CHUNKS, CHUNKS + finish_lag - 1, after, 0)

    corners = [links_used(i // 4, i // 2 % 2, i % 2) for i in range(4 * DEPTH)]
    corner = zz * 4 + y * 2 + x
    for link in range(4):
        counts = [used[link] for used in corners]
        used = pick(corner, counts)
        for count in sorted(set(counts) - {0}):

            @pl.when(used == count)
            def _():
                bulk(hid.at[pl.ds(0, count)], sent.at[link]).wait_send()

    bulk(part, far_sent.at[0]).wait_send()

    @pl.when(jnp.logical_not(is_source))
    def _():
        bulk(staged, pair_sent.at[0]).wait_send()
        bulk(stats.at[:, pl.ds(1, n - 1)], stat_sent.at[s]).wait_send()
        bulk(stats, stat_sent.at[1 - s]).wait_send()

    finish(CHUNKS - 1)


def product_kernel(total, last, term, loss_in, out, loss_out, rounded, sem):
    half_n = total.shape[0]
    right = term[pl.ds(CHUNKS - 2, 2)].reshape(last.shape[2], term.shape[2])

    def copy(k):
        return pltpu.make_async_copy(rounded.at[k], out.at[k], sem.at[k])

    def one(k, carry):
        rounded[k] = (total[k] + jnp.dot(last[k], right, preferred_element_type=jnp.float32)).astype(out.dtype)
        copy(k).start()
        return carry

    lax.fori_loop(0, half_n, one, 0)
    for g in range(GROUPS):
        loss_out[g * LANES : (g + 1) * LANES] = loss_in[g, 0]

    def settle(k, carry):
        copy(k).wait()
        return carry

    lax.fori_loop(0, half_n, settle, 0)


def relayed(n, hidden, weight, tangent, targets):
    half_n = n // 2
    tokens_own, shard = hidden.shape
    width = weight.shape[1]
    rows = 2 * tokens_own // CHUNKS
    blocks = (half_n, shard, width)
    hbm = pl.BlockSpec(memory_space=pltpu.HBM)
    vmem = pl.BlockSpec(memory_space=pltpu.VMEM)
    dma = pltpu.SemaphoreType.DMA
    total, last, term, loss = pl.pallas_call(
        functools.partial(gather_kernel, n),
        name="gather_logits",
        out_shape=(
            pltpu.VMEM(blocks, jnp.float32),
            pltpu.VMEM((half_n, shard, 2 * rows), hidden.dtype),
            pltpu.VMEM((CHUNKS, rows, width), jnp.bfloat16),
            pltpu.VMEM((GROUPS, 1, rows), jnp.float32),
        ),
        in_specs=[hbm, hbm, hbm, hbm],
        out_specs=(vmem, vmem, vmem, vmem),
        scratch_shapes=[
            pltpu.VMEM((half_n * CHUNKS, rows, shard), hidden.dtype),
            pltpu.VMEM((half_n, shard, (CHUNKS - 2) * rows), hidden.dtype),
            pltpu.VMEM((CHUNKS, rows // 2, shard), hidden.dtype),
            pltpu.VMEM(blocks, weight.dtype),
            pltpu.VMEM(blocks, tangent.dtype),
            pltpu.VMEM((CHUNKS, rows, 2 * width), jnp.float32),
            pltpu.VMEM((CHUNKS, rows, 2 * width), jnp.float32),
            pltpu.VMEM((CHUNKS, n, 4, rows), jnp.float32),
            pltpu.VMEM((1, tokens_own), jnp.int32),
            pltpu.VMEM((1, tokens_own), jnp.int32),
            pltpu.VMEM((CHUNKS, rows, LANES), jnp.int32),
            dma((half_n, CHUNKS)),
            dma((4,)),
            dma((CHUNKS,)),
            dma((1,)),
            dma((4,)),
            dma((1,)),
            dma((CHUNKS,)),
            dma((2,)),
            dma((CHUNKS,)),
            dma((2,)),
            pltpu.SemaphoreType.REGULAR((5,)),
        ],
        compiler_params=pltpu.CompilerParams(
            collective_id=0, has_side_effects=True, vmem_limit_bytes=42 * 2**20
        ),
    )(
        pltpu.with_memory_space_constraint(hidden.reshape(CHUNKS, rows // 2, shard), pltpu.HBM),
        pltpu.with_memory_space_constraint(weight.reshape(blocks), pltpu.HBM),
        pltpu.with_memory_space_constraint(tangent.reshape(blocks), pltpu.HBM),
        pltpu.with_memory_space_constraint(targets.reshape(1, tokens_own), pltpu.HBM),
    )
    ggn, token_loss = pl.pallas_call(
        product_kernel,
        name="product",
        out_shape=(
            jax.ShapeDtypeStruct(blocks, jnp.bfloat16),
            jax.ShapeDtypeStruct((tokens_own,), jnp.float32),
        ),
        in_specs=[vmem, vmem, vmem, vmem],
        out_specs=(hbm, vmem),
        scratch_shapes=[pltpu.VMEM(blocks, jnp.bfloat16), dma((half_n,))],
        compiler_params=pltpu.CompilerParams(vmem_limit_bytes=20 * 2**20),
    )(total, last, term, loss)
    return ggn.reshape(weight.shape), token_loss


def partner(value, axis, stride):
    mask = 2**stride
    pairs = [(source, source ^ mask) for source in range(lax.axis_size(axis))]
    return lax.ppermute(value, axis, pairs)


def on_device(hidden, weight, tangent, targets):
    n = lax.axis_size("vocab")
    if n == PLANE * DEPTH and lax.axis_size("seq") == 2 and hidden.shape[0] == LANES * GROUPS and hidden.shape[1] % LANES == 0:
        return relayed(n, hidden, weight, tangent, targets)
    vocab_index = lax.axis_index("vocab")
    shard_width = weight.shape[1]
    half_width = weight.shape[0]
    whole = lax.all_gather(hidden, "vocab", axis=1, tiled=True)
    seq_index = lax.axis_index("seq")
    own_part = lax.dynamic_slice_in_dim(whole, seq_index * half_width, half_width, 1)
    far_part = lax.dynamic_slice_in_dim(whole, (1 - seq_index) * half_width, half_width, 1)
    received = partner(far_part, "seq", 0)
    leading = jnp.where(seq_index == 0, own_part, received)
    trailing = jnp.where(seq_index == 0, received, own_part)
    stacked = jnp.concatenate([leading, trailing], axis=0)
    partial_logits = jnp.dot(stacked, weight, preferred_element_type=jnp.float32)
    partial_tangent = jnp.dot(stacked, tangent, preferred_element_type=jnp.float32)
    logits, tangent_logits = (
        lax.psum_scatter(partial_logits, "seq", scatter_dimension=0, tiled=True),
        lax.psum_scatter(partial_tangent, "seq", scatter_dimension=0, tiled=True),
    )
    local_target = targets - vocab_index * shard_width
    columns_ids = jnp.arange(shard_width, dtype=jnp.int32)
    picked_local = jnp.sum(
        jnp.where(columns_ids[None, :] == local_target[:, None], logits, jnp.float32(0.0)), axis=1
    )
    local_top = jnp.max(logits, axis=1)
    row_top = lax.pmax(local_top, "vocab")
    exp_logits = jnp.exp(logits - row_top[:, None])
    totals, tangent_sum, picked = lax.psum(
        (jnp.sum(exp_logits, axis=1), jnp.sum(exp_logits * tangent_logits, axis=1), picked_local),
        "vocab",
    )
    expect = tangent_sum / totals
    token_loss = row_top + jnp.log(totals) - picked
    weight_term = (exp_logits / totals[:, None] * (tangent_logits - expect[:, None])).astype(
        jnp.bfloat16
    )
    far_term = partner(weight_term, "seq", 0)
    lead_term = jnp.where(seq_index == 0, weight_term, far_term)
    trail_term = jnp.where(seq_index == 0, far_term, weight_term)
    all_terms = jnp.concatenate([lead_term, trail_term], axis=0)
    ggn = jnp.einsum("td,tv->dv", stacked, all_terms, preferred_element_type=jnp.float32).astype(
        jnp.bfloat16
    )
    return (ggn, token_loss)


def solution(mesh):
    in_specs = (P("seq", "vocab"), P("seq", "vocab"), P("seq", "vocab"), P("seq"))
    out_specs = (P("seq", "vocab"), P("seq"))
    return jax.shard_map(
        on_device, mesh=mesh, in_specs=in_specs, out_specs=out_specs, check_vma=False
    )
```

```python
import functools

import jax
import jax.numpy as jnp
from jax import lax
from jax.experimental import pallas as pl
from jax.experimental.pallas import tpu as pltpu
from jax.sharding import PartitionSpec as P

MESH = pl.DeviceIdType.MESH
PLANE, DEPTH = 4, 4
CHUNKS = 8
GROUPS = CHUNKS // 2
LEAD = 3
LAGS = ((0, 0, 0, 3, 0, 2, 1, 5), (0, 1, 1, 3, 3, 4, 4, 5), (0, 0, 2, 2, 2, 3, 4, 5), (0, 0, 2, 2, 2, 3, 5, 5))
ORDERS = ((5, 2, 7, 4, 1, 3, 6, 0), (5, 3, 0, 4, 1, 6, 7, 2), (5, 0, 2, 4, 7, 1, 6, 3), (6, 5, 7, 2, 0, 3, 1, 4))
TALL = (78, 18, 144, 0, 129, 44, 176, 224)
DEEP = (4, 0, 1, 1, 0, 0, 0, 0)
VIA = (30, 12, 167, 159, 99, 142, 22, 95)
FINISH_LAGS = (8, 8, 4, 4)
LANES = 128


def links_used(zz, y, x):
    used = [0, 0, 0, 0]
    for c in range(CHUNKS):
        for item in range(8):
            szz, dy, dx = item // 4, item // 2 % 2, item % 2
            spot = (y + dy) % 2 * 2 + (x + dx) % 2
            tall = TALL[c] >> (szz * 4 + spot) & 1
            deep = DEEP[c] >> spot & 1 and szz == 1
            via = VIA[c] >> (szz * 4 + spot) & 1
            column = dx + dy == 0
            inplane = not (zz > szz and tall or zz < szz and deep)
            used[0] += inplane and (column or (dx == 0 and dy == 1 and via == 1))
            used[1] += inplane and (column or (dx == 1 and dy == 0 and via == 0))
            used[2] += (column or tall) and zz >= szz and zz < DEPTH - 1
            used[3] += (column or deep) and zz == 1 and szz == 1
    return [int(u) for u in used]


def packed(values, bits):
    word = sum(value << (bits * i) for i, value in enumerate(values))
    return word - (word >> 31 << 32)


def pick(index, values):
    chosen = jnp.int32(values[0])
    for i, value in enumerate(values[1:]):
        chosen = jnp.where(index == i + 1, jnp.int32(value), chosen)
    return chosen


def field(word, index, bits):
    return (word >> (index * bits)) & (2**bits - 1)


def gather_kernel(
    n, hidden, weight, tangent, targets, total, last, term, loss_out,
    hid, flipped, staged, both_w, part, far, stats, target, target_pair, wanted,
    recv, sent, pair_recv, pair_sent, load_sem, far_sent, far_recv,
    stat_sent, stat_recv, target_sem,
):
    s = lax.axis_index("seq")
    v = lax.axis_index("vocab")
    half_n = n // 2
    rows = hid.shape[1]
    half = rows // 2
    group_rows = 2 * rows
    width = weight.shape[2]
    z, y, x = v // PLANE, (v // 2) % 2, v % 2
    zz = z + s * (DEPTH - 1 - 2 * z)
    up_step = PLANE * (1 - 2 * s)
    x_dev = (s, v + 1 - 2 * x)
    y_dev = (s, v + 2 - 4 * y)
    up_dev = (s, v + up_step)
    down_dev = (s, v - up_step)
    pair_dev = (1 - s, v)
    is_source = zz < DEPTH // 2
    has_up = zz < DEPTH - 1
    has_down = zz > 0
    along_count = has_up.astype(jnp.int32) + has_down.astype(jnp.int32)
    own_k = jnp.where(is_source, v - half_n * s, 0)
    pair_k = jnp.where(is_source, 0, v - half_n * (1 - s))
    lag_word = pick(zz, [packed(lags, 4) for lags in LAGS])
    order_word = pick(zz, [packed(order, 3) for order in ORDERS])
    last_lag = pick(zz, [max(lags) for lags in LAGS])
    finish_lag = pick(zz, FINISH_LAGS)

    mine = pl.ds(pl.multiple_of(s * half, half), half)
    theirs = pl.ds(pl.multiple_of((1 - s) * half, half), half)

    load_w = pltpu.make_async_copy(weight, both_w.at[:, :, pl.ds(0, width)], load_sem.at[0])
    load_t = pltpu.make_async_copy(tangent, both_w.at[:, :, pl.ds(width, width)], load_sem.at[1])
    load_target = pltpu.make_async_copy(targets, target, load_sem.at[2])

    own_load = pltpu.make_async_copy(hidden, hid.at[pl.ds(own_k * CHUNKS, CHUNKS), mine], load_sem.at[3])
    stage = pltpu.make_async_copy(hidden, staged, load_sem.at[3])

    def pair_copy(k, c, span):
        return pltpu.make_async_remote_copy(
            src_ref=staged.at[c],
            dst_ref=hid.at[k * CHUNKS + c, span],
            send_sem=pair_sent.at[0],
            recv_sem=pair_recv.at[c],
            device_id=pair_dev,
            device_id_type=MESH,
        )

    def bulk(ref, semaphore):
        return pltpu.make_async_remote_copy(
            src_ref=ref,
            dst_ref=ref,
            send_sem=semaphore,
            recv_sem=semaphore,
            device_id=pair_dev,
            device_id_type=MESH,
        )

    def greet(semaphore, device):
        pl.semaphore_signal(semaphore, inc=1, device_id=device, device_id_type=MESH)

    def greet_along(semaphore):
        @pl.when(has_up)
        def _():
            greet(semaphore, up_dev)

        @pl.when(has_down)
        def _():
            greet(semaphore, down_dev)

    barrier = pltpu.get_barrier_semaphore()
    greet(barrier, pair_dev)
    greet(barrier, x_dev)
    greet(barrier, y_dev)
    greet_along(barrier)

    @pl.when(is_source)
    def _():
        own_load.start()

    @pl.when(jnp.logical_not(is_source))
    def _():
        stage.start()

    load_target.start()
    load_w.start()
    load_t.start()

    def clear(i, carry):
        part[i] = jnp.zeros(part.shape[1:], jnp.float32)
        return carry

    lax.fori_loop(0, CHUNKS, clear, 0)
    loss_out[...] = jnp.zeros_like(loss_out)
    load_target.wait()
    pl.semaphore_wait(barrier, 3 + along_count)
    pair_target = pltpu.make_async_remote_copy(
        src_ref=target,
        dst_ref=target_pair,
        send_sem=target_sem.at[0],
        recv_sem=target_sem.at[1],
        device_id=pair_dev,
        device_id_type=MESH,
    )
    pair_target.start()

    @pl.when(jnp.logical_not(is_source))
    def _():
        stage.wait()

        def give(c, carry):
            pair_copy(pair_k, c, mine).start()
            return carry

        lax.fori_loop(0, CHUNKS, give, 0)

    @pl.when(is_source)
    def _():
        own_load.wait()

    def copy(link, k, c, device, span):
        piece = hid.at[k * CHUNKS + c, span]
        return pltpu.make_async_remote_copy(
            src_ref=piece,
            dst_ref=piece,
            send_sem=sent.at[link],
            recv_sem=recv.at[k, c],
            device_id=device,
            device_id_type=MESH,
        )

    def routes(k, c, dx, dy, szz, span):
        column = dx + dy == 0
        spot = ((y + dy) % 2) * 2 + (x + dx) % 2
        word = pick(c, [TALL[i] | VIA[i] << 8 | DEEP[i] << 20 for i in range(CHUNKS)])
        place = szz * 4 + spot
        tall = field(word, place, 1) == 1
        via = field(word, place + 8, 1)
        deep = field(word, place + 16, 1) == 1
        along = jnp.logical_or(
            jnp.logical_and(zz > szz, tall), jnp.logical_and(zz < szz, deep)
        )
        inplane = jnp.logical_not(along)
        via_x = jnp.logical_and(jnp.logical_and(dx == 0, dy == 1), via == 1)
        via_y = jnp.logical_and(jnp.logical_and(dx == 1, dy == 0), via == 0)
        go_up = jnp.logical_and(jnp.logical_or(column, tall), jnp.logical_and(zz >= szz, has_up))
        go_down = jnp.logical_and(jnp.logical_or(column, deep), jnp.logical_and(zz == 1, szz == 1))
        return (
            (go_up, copy(2, k, c, up_dev, span)),
            (go_down, copy(3, k, c, down_dev, span)),
            (jnp.logical_and(inplane, jnp.logical_or(column, via_x)), copy(0, k, c, x_dev, span)),
            (jnp.logical_and(inplane, jnp.logical_or(column, via_y)), copy(1, k, c, y_dev, span)),
        )

    def forward(k, c, dx, dy, szz, span):
        for condition, route in routes(k, c, dx, dy, szz, span):
            @pl.when(condition)
            def _():
                route.start()

    everything = pl.ds(0, rows)

    def item(q):
        r, i = q // 2, q % 2
        dx, dy = r % 2, r // 2
        first = jnp.where(zz >= 1, 1, 0)
        szz = first + i * (1 - 2 * first)
        src_z = szz + s * (DEPTH - 1 - 2 * szz)
        k = src_z * PLANE + ((y + dy) % 2) * 2 + (x + dx) % 2 - half_n * s
        return k, dx, dy, szz

    def send_own(c):
        @pl.when(jnp.logical_and(is_source, c < CHUNKS))
        def _():
            forward(own_k, c, 0, 0, zz, mine)
            pair_copy(own_k, c, theirs).wait_recv()
            forward(own_k, c, 0, 0, zz, theirs)

    def lead(c, carry):
        send_own(c)
        return carry

    lax.fori_loop(0, LEAD, lead, 0)

    pair_target.wait()

    @pl.when(jnp.logical_not(is_source))
    def _():
        for g in range(GROUPS):
            for ids, side in ((target, mine), (target_pair, theirs)):
                upright = jnp.broadcast_to(ids[:, g * rows : (g + 1) * rows], (LANES, rows)).T
                wanted[2 * g, side, :] = upright[:half]
                wanted[2 * g + 1, side, :] = upright[half:]

    load_w.wait()
    load_t.wait()

    def far_copy(c):
        return pltpu.make_async_remote_copy(
            src_ref=part.at[c],
            dst_ref=far.at[c],
            send_sem=far_sent.at[0],
            recv_sem=far_recv.at[c],
            device_id=pair_dev,
            device_id_type=MESH,
        )

    def stat_copy(c, core, d):
        return pltpu.make_async_remote_copy(
            src_ref=stats.at[c, 0],
            dst_ref=stats.at[c, d],
            send_sem=stat_sent.at[core],
            recv_sem=stat_recv.at[c],
            device_id=(core, (v + d) % n),
            device_id_type=MESH,
        )

    def local_stats(c):
        far_copy(c).wait_recv()

        both = part[c] + far[c]
        logits, slope = both[:, :width], both[:, width:]
        top = jnp.max(logits, axis=1, keepdims=True)
        e = jnp.exp(logits - top)
        amount = jnp.sum(e, axis=1, keepdims=True)
        weighted = jnp.sum(e * slope, axis=1, keepdims=True)
        columns = lax.broadcasted_iota(jnp.int32, logits.shape, 1) + v * width
        picked = jnp.sum(jnp.where(columns == wanted[c][:, 0:1], logits, 0.0), axis=1, keepdims=True)
        lane = lax.broadcasted_iota(jnp.int32, (rows, LANES), 1)
        packed = jnp.where(lane == 0, top, jnp.where(lane == 1, amount, jnp.where(lane == 2, weighted, picked)))
        stats[c, 0] = packed.T[:4]

        stat_copy(c, 1 - s, 0).start()

        def start(d, carry):
            stat_copy(c, 0, n - d).start()
            stat_copy(c, 1, n - d).start()
            return carry

        lax.fori_loop(1, n, start, 0)

    def finish(c):
        @pl.when(is_source)
        def _():
            far_copy(c).wait_recv()
            bulk(stats.at[c], stat_recv.at[c]).wait_recv()

        @pl.when(jnp.logical_not(is_source))
        def _():
            bulk(stats.at[c, pl.ds(1, n - 1)], stat_recv.at[c]).wait_recv()

        every = stats[c]
        tops = every[:, 0, :]
        row_top = jnp.max(tops, axis=0, keepdims=True)
        scale = jnp.exp(tops - row_top)
        totals = jnp.sum(scale * every[:, 1, :], axis=0, keepdims=True)
        tangent_sum = jnp.sum(scale * every[:, 2, :], axis=0, keepdims=True)
        picked = jnp.sum(every[:, 3, :], axis=0, keepdims=True)
        expect = tangent_sum / totals
        line = lax.broadcasted_iota(jnp.int32, (LANES, rows), 0)
        side = jnp.where(line == 0, row_top, jnp.where(line == 1, totals, expect)).T
        both = part[c] + far[c]
        value = jnp.exp(both[:, :width] - side[:, 0:1]) / side[:, 1:2] * (both[:, width:] - side[:, 2:3])
        term[c] = value.astype(term.dtype)
        loss = row_top + jnp.log(totals) - picked
        place = c % 2
        loss = jnp.where(place == s, loss, pltpu.roll(loss, half, 1))
        lane = lax.broadcasted_iota(jnp.int32, (1, rows), 1)
        kept = loss_out[c // 2]
        loss_out[c // 2] = jnp.where(lane // half == place, loss, kept)

    early = 2 * group_rows

    def product(first, second, k):
        @pl.when(first)
        def _():
            right = term[pl.ds(0, 4)].reshape(early, width)
            total[k] = jnp.dot(flipped[k, :, pl.ds(0, early)], right, preferred_element_type=jnp.float32)

        @pl.when(second)
        def _():
            right = term[pl.ds(4, 2)].reshape(group_rows, width)
            left = flipped[k, :, pl.ds(early, group_rows)]
            total[k] += jnp.dot(left, right, preferred_element_type=jnp.float32)

    def product_due(done):
        return done == finish_lag + 4, done == finish_lag + 6

    def ripe(done, act):
        single = done >= CHUNKS - 2
        whole = jnp.logical_and(done >= 0, done % 2 == 1)
        valid = jnp.logical_and(done < CHUNKS, jnp.logical_or(single, whole))

        def one(c, carry):
            act(c)
            return carry

        @pl.when(valid)
        def _():
            lax.fori_loop(jnp.where(single, done, done - 1), done + 1, one, 0)

    def stages(done):
        @pl.when(jnp.logical_not(is_source))
        def _():
            ripe(done, local_stats)

        ripe(done - finish_lag, finish)

    def step(t, carry):
        done = t - last_lag

        send_own(t + LEAD)
        first, second = product_due(done)

        def one(i, inner):
            q = field(order_word, i, 3)
            c = t - field(lag_word, q, 4)

            @pl.when(jnp.logical_and(c >= 0, c < CHUNKS))
            def _():
                k, dx, dy, szz = item(q)
                own = jnp.logical_and(dx + dy == 0, szz == zz)

                @pl.when(jnp.logical_not(own))
                def _():
                    copy(0, k, c, x_dev, everything).wait_recv()
                    forward(k, c, dx, dy, szz, everything)

                @pl.when(jnp.logical_and(c < CHUNKS - 2, c % 2 == 1))
                def _():
                    two = hid[pl.ds(k * CHUNKS + c - 1, 2)].reshape(group_rows, hid.shape[2])
                    more = jnp.dot(two, both_w[k], preferred_element_type=jnp.float32)
                    part[pl.ds(c - 1, 2)] += more.reshape(2, rows, 2 * width)
                    flipped[k, :, pl.ds(pl.multiple_of((c - 1) * rows, group_rows), group_rows)] = two.T

                @pl.when(c >= CHUNKS - 2)
                def _():
                    part[c] += jnp.dot(hid[k * CHUNKS + c], both_w[k], preferred_element_type=jnp.float32)
                    at = (c - CHUNKS + 2) * rows
                    last[k, :, pl.ds(pl.multiple_of(at, rows), rows)] = hid[k * CHUNKS + c].T

            product(first, second, i)
            return inner

        lax.fori_loop(0, 8, one, 0)

        ripe(done, lambda c: far_copy(c).start())
        stages(done)
        return carry

    lax.fori_loop(0, CHUNKS + last_lag, step, 0)

    def after(done, carry):
        stages(done)
        first, second = product_due(done)

        @pl.when(jnp.logical_or(first, second))
        def _():
            def one(k, inner):
                product(first, second, k)
                return inner

            lax.fori_loop(0, half_n, one, 0)

        return carry

    lax.fori_loop(CHUNKS, CHUNKS + finish_lag - 1, after, 0)

    corners = [links_used(i // 4, i // 2 % 2, i % 2) for i in range(4 * DEPTH)]
    corner = zz * 4 + y * 2 + x
    for link in range(4):
        counts = [used[link] for used in corners]
        used = pick(corner, counts)
        for count in sorted(set(counts) - {0}):

            @pl.when(used == count)
            def _():
                bulk(hid.at[pl.ds(0, count)], sent.at[link]).wait_send()

    bulk(part, far_sent.at[0]).wait_send()

    @pl.when(jnp.logical_not(is_source))
    def _():
        bulk(staged, pair_sent.at[0]).wait_send()
        bulk(stats.at[:, pl.ds(1, n - 1)], stat_sent.at[s]).wait_send()
        bulk(stats, stat_sent.at[1 - s]).wait_send()

    finish(CHUNKS - 1)


def product_kernel(total, last, term, loss_in, out, loss_out, rounded, sem):
    half_n = total.shape[0]
    right = term[pl.ds(CHUNKS - 2, 2)].reshape(last.shape[2], term.shape[2])

    def copy(k):
        return pltpu.make_async_copy(rounded.at[k], out.at[k], sem.at[k])

    def one(k, carry):
        rounded[k] = (total[k] + jnp.dot(last[k], right, preferred_element_type=jnp.float32)).astype(out.dtype)
        copy(k).start()
        return carry

    lax.fori_loop(0, half_n, one, 0, unroll=4)
    for g in range(GROUPS):
        loss_out[g * LANES : (g + 1) * LANES] = loss_in[g, 0]

    def settle(k, carry):
        copy(k).wait()
        return carry

    lax.fori_loop(0, half_n, settle, 0)


def relayed(n, hidden, weight, tangent, targets):
    half_n = n // 2
    tokens_own, shard = hidden.shape
    width = weight.shape[1]
    rows = 2 * tokens_own // CHUNKS
    blocks = (half_n, shard, width)
    hbm = pl.BlockSpec(memory_space=pltpu.HBM)
    vmem = pl.BlockSpec(memory_space=pltpu.VMEM)
    dma = pltpu.SemaphoreType.DMA
    total, last, term, loss = pl.pallas_call(
        functools.partial(gather_kernel, n),
        name="gather_logits",
        out_shape=(
            pltpu.VMEM(blocks, jnp.float32),
            pltpu.VMEM((half_n, shard, 2 * rows), hidden.dtype),
            pltpu.VMEM((CHUNKS, rows, width), jnp.bfloat16),
            pltpu.VMEM((GROUPS, 1, rows), jnp.float32),
        ),
        in_specs=[hbm, hbm, hbm, hbm],
        out_specs=(vmem, vmem, vmem, vmem),
        scratch_shapes=[
            pltpu.VMEM((half_n * CHUNKS, rows, shard), hidden.dtype),
            pltpu.VMEM((half_n, shard, (CHUNKS - 2) * rows), hidden.dtype),
            pltpu.VMEM((CHUNKS, rows // 2, shard), hidden.dtype),
            pltpu.VMEM((half_n, shard, 2 * width), weight.dtype),
            pltpu.VMEM((CHUNKS, rows, 2 * width), jnp.float32),
            pltpu.VMEM((CHUNKS, rows, 2 * width), jnp.float32),
            pltpu.VMEM((CHUNKS, n, 4, rows), jnp.float32),
            pltpu.VMEM((1, tokens_own), jnp.int32),
            pltpu.VMEM((1, tokens_own), jnp.int32),
            pltpu.VMEM((CHUNKS, rows, LANES), jnp.int32),
            dma((half_n, CHUNKS)),
            dma((4,)),
            dma((CHUNKS,)),
            dma((1,)),
            dma((4,)),
            dma((1,)),
            dma((CHUNKS,)),
            dma((2,)),
            dma((CHUNKS,)),
            dma((2,)),
        ],
        compiler_params=pltpu.CompilerParams(
            collective_id=0, has_side_effects=True, vmem_limit_bytes=42 * 2**20
        ),
    )(
        pltpu.with_memory_space_constraint(hidden.reshape(CHUNKS, rows // 2, shard), pltpu.HBM),
        pltpu.with_memory_space_constraint(weight.reshape(blocks), pltpu.HBM),
        pltpu.with_memory_space_constraint(tangent.reshape(blocks), pltpu.HBM),
        pltpu.with_memory_space_constraint(targets.reshape(1, tokens_own), pltpu.HBM),
    )
    ggn, token_loss = pl.pallas_call(
        product_kernel,
        name="product",
        out_shape=(
            jax.ShapeDtypeStruct(blocks, jnp.bfloat16),
            jax.ShapeDtypeStruct((tokens_own,), jnp.float32),
        ),
        in_specs=[vmem, vmem, vmem, vmem],
        out_specs=(hbm, vmem),
        scratch_shapes=[pltpu.VMEM(blocks, jnp.bfloat16), dma((half_n,))],
        compiler_params=pltpu.CompilerParams(vmem_limit_bytes=20 * 2**20),
    )(total, last, term, loss)
    return ggn.reshape(weight.shape), token_loss


def partner(value, axis, stride):
    mask = 2**stride
    pairs = [(source, source ^ mask) for source in range(lax.axis_size(axis))]
    return lax.ppermute(value, axis, pairs)


def on_device(hidden, weight, tangent, targets):
    n = lax.axis_size("vocab")
    if n == PLANE * DEPTH and lax.axis_size("seq") == 2 and hidden.shape[0] == LANES * GROUPS and hidden.shape[1] % LANES == 0:
        return relayed(n, hidden, weight, tangent, targets)
    vocab_index = lax.axis_index("vocab")
    shard_width = weight.shape[1]
    half_width = weight.shape[0]
    whole = lax.all_gather(hidden, "vocab", axis=1, tiled=True)
    seq_index = lax.axis_index("seq")
    own_part = lax.dynamic_slice_in_dim(whole, seq_index * half_width, half_width, 1)
    far_part = lax.dynamic_slice_in_dim(whole, (1 - seq_index) * half_width, half_width, 1)
    received = partner(far_part, "seq", 0)
    leading = jnp.where(seq_index == 0, own_part, received)
    trailing = jnp.where(seq_index == 0, received, own_part)
    stacked = jnp.concatenate([leading, trailing], axis=0)
    partial_logits = jnp.dot(stacked, weight, preferred_element_type=jnp.float32)
    partial_tangent = jnp.dot(stacked, tangent, preferred_element_type=jnp.float32)
    logits, tangent_logits = (
        lax.psum_scatter(partial_logits, "seq", scatter_dimension=0, tiled=True),
        lax.psum_scatter(partial_tangent, "seq", scatter_dimension=0, tiled=True),
    )
    local_target = targets - vocab_index * shard_width
    columns_ids = jnp.arange(shard_width, dtype=jnp.int32)
    picked_local = jnp.sum(
        jnp.where(columns_ids[None, :] == local_target[:, None], logits, jnp.float32(0.0)), axis=1
    )
    local_top = jnp.max(logits, axis=1)
    row_top = lax.pmax(local_top, "vocab")
    exp_logits = jnp.exp(logits - row_top[:, None])
    totals, tangent_sum, picked = lax.psum(
        (jnp.sum(exp_logits, axis=1), jnp.sum(exp_logits * tangent_logits, axis=1), picked_local),
        "vocab",
    )
    expect = tangent_sum / totals
    token_loss = row_top + jnp.log(totals) - picked
    weight_term = (exp_logits / totals[:, None] * (tangent_logits - expect[:, None])).astype(
        jnp.bfloat16
    )
    far_term = partner(weight_term, "seq", 0)
    lead_term = jnp.where(seq_index == 0, weight_term, far_term)
    trail_term = jnp.where(seq_index == 0, far_term, weight_term)
    all_terms = jnp.concatenate([lead_term, trail_term], axis=0)
    ggn = jnp.einsum("td,tv->dv", stacked, all_terms, preferred_element_type=jnp.float32).astype(
        jnp.bfloat16
    )
    return (ggn, token_loss)


def solution(mesh):
    in_specs = (P("seq", "vocab"), P("seq", "vocab"), P("seq", "vocab"), P("seq"))
    out_specs = (P("seq", "vocab"), P("seq"))
    return jax.shard_map(
        on_device, mesh=mesh, in_specs=in_specs, out_specs=out_specs, check_vma=False
    )
```

```python
import functools

import jax
import jax.numpy as jnp
from jax import lax
from jax.experimental import pallas as pl
from jax.experimental.pallas import tpu as pltpu
from jax.sharding import PartitionSpec as P

MESH = pl.DeviceIdType.MESH
PLANE, DEPTH = 4, 4
CHUNKS = 8
GROUPS = CHUNKS // 2
LEAD = 4
LAGS = ((0, 0, 1, 4, 0, 3, 4, 5), (0, 0, 1, 3, 1, 3, 4, 5), (0, 0, 2, 2, 2, 3, 5, 5), (0, 0, 2, 3, 3, 3, 5, 5))
ORDERS = ((5, 0, 6, 3, 4, 1, 7, 2), (0, 3, 2, 5, 4, 6, 1, 7), (6, 5, 0, 1, 4, 7, 2, 3), (4, 5, 3, 0, 2, 6, 7, 1))
TALL = (156, 62, 1, 4, 8, 40, 67, 72)
DEEP = (4, 0, 0, 1, 0, 0, 0, 0)
VIA = (133, 200, 63, 62, 116, 28, 123, 1)
FINISH_LAG = 4
FINISHED = (CHUNKS - FINISH_LAG) // 2
LANES = 128
UNROLL = 4


def links_used(zz, y, x):
    used = [0, 0, 0, 0]
    for c in range(CHUNKS):
        for item in range(8):
            szz, dy, dx = item // 4, item // 2 % 2, item % 2
            spot = (y + dy) % 2 * 2 + (x + dx) % 2
            tall = TALL[c] >> (szz * 4 + spot) & 1
            deep = DEEP[c] >> spot & 1 and szz == 1
            via = VIA[c] >> (szz * 4 + spot) & 1
            column = dx + dy == 0
            inplane = not (zz > szz and tall or zz < szz and deep)
            used[0] += inplane and (column or (dx == 0 and dy == 1 and via == 1))
            used[1] += inplane and (column or (dx == 1 and dy == 0 and via == 0))
            used[2] += (column or tall) and zz >= szz and zz < DEPTH - 1
            used[3] += (column or deep) and zz == 1 and szz == 1
    return [int(u) for u in used]


def packed(values, bits):
    word = sum(value << (bits * i) for i, value in enumerate(values))
    return word - (word >> 31 << 32)


def pick(index, values):
    chosen = jnp.int32(values[0])
    for i, value in enumerate(values[1:]):
        chosen = jnp.where(index == i + 1, jnp.int32(value), chosen)
    return chosen


def field(word, index, bits):
    return (word >> (index * bits)) & (2**bits - 1)


def gather_kernel(
    n, hidden, weight, tangent, targets, total, last, term, loss_out,
    hid, flipped, staged, both_w, part, far, stats, target, target_pair, wanted,
    recv, sent, pair_recv, pair_sent, load_sem, far_sent, far_recv,
    stat_sent, stat_recv, target_sem,
):
    s = lax.axis_index("seq")
    v = lax.axis_index("vocab")
    half_n = n // 2
    rows = hid.shape[1]
    half = rows // 2
    group_rows = 2 * rows
    width = weight.shape[2]
    z, y, x = v // PLANE, (v // 2) % 2, v % 2
    zz = z + s * (DEPTH - 1 - 2 * z)
    up_step = PLANE * (1 - 2 * s)
    x_dev = (s, v + 1 - 2 * x)
    y_dev = (s, v + 2 - 4 * y)
    up_dev = (s, v + up_step)
    down_dev = (s, v - up_step)
    pair_dev = (1 - s, v)
    is_source = zz < DEPTH // 2
    has_up = zz < DEPTH - 1
    has_down = zz > 0
    along_count = has_up.astype(jnp.int32) + has_down.astype(jnp.int32)
    own_k = jnp.where(is_source, v - half_n * s, 0)
    pair_k = jnp.where(is_source, 0, v - half_n * (1 - s))
    lag_word = pick(zz, [packed(lags, 4) for lags in LAGS])
    order_word = pick(zz, [packed(order, 3) for order in ORDERS])
    last_lag = pick(zz, [max(lags) for lags in LAGS])

    mine = pl.ds(pl.multiple_of(s * half, half), half)
    theirs = pl.ds(pl.multiple_of((1 - s) * half, half), half)

    load_w = pltpu.make_async_copy(weight, both_w.at[:, :, pl.ds(0, width)], load_sem.at[0])
    load_t = pltpu.make_async_copy(tangent, both_w.at[:, :, pl.ds(width, width)], load_sem.at[1])
    load_target = pltpu.make_async_copy(targets, target, load_sem.at[2])

    own_load = pltpu.make_async_copy(hidden, hid.at[pl.ds(own_k * CHUNKS, CHUNKS), mine], load_sem.at[3])
    stage = pltpu.make_async_copy(hidden, staged, load_sem.at[3])

    def pair_copy(k, c, span):
        return pltpu.make_async_remote_copy(
            src_ref=staged.at[c],
            dst_ref=hid.at[k * CHUNKS + c, span],
            send_sem=pair_sent.at[0],
            recv_sem=pair_recv.at[c],
            device_id=pair_dev,
            device_id_type=MESH,
        )

    def bulk(ref, semaphore):
        return pltpu.make_async_remote_copy(
            src_ref=ref,
            dst_ref=ref,
            send_sem=semaphore,
            recv_sem=semaphore,
            device_id=pair_dev,
            device_id_type=MESH,
        )

    def greet(semaphore, device):
        pl.semaphore_signal(semaphore, inc=1, device_id=device, device_id_type=MESH)

    def greet_along(semaphore):
        @pl.when(has_up)
        def _():
            greet(semaphore, up_dev)

        @pl.when(has_down)
        def _():
            greet(semaphore, down_dev)

    barrier = pltpu.get_barrier_semaphore()
    greet(barrier, pair_dev)
    greet(barrier, x_dev)
    greet(barrier, y_dev)
    greet_along(barrier)

    @pl.when(is_source)
    def _():
        own_load.start()

    @pl.when(jnp.logical_not(is_source))
    def _():
        stage.start()

    load_target.start()
    load_w.start()
    load_t.start()

    def clear(i, carry):
        part[i] = jnp.zeros(part.shape[1:], jnp.float32)
        return carry

    lax.fori_loop(0, CHUNKS, clear, 0)
    load_target.wait()
    pl.semaphore_wait(barrier, 3 + along_count)
    pair_target = pltpu.make_async_remote_copy(
        src_ref=target,
        dst_ref=target_pair,
        send_sem=target_sem.at[0],
        recv_sem=target_sem.at[1],
        device_id=pair_dev,
        device_id_type=MESH,
    )
    pair_target.start()

    @pl.when(jnp.logical_not(is_source))
    def _():
        stage.wait()

        def give(c, carry):
            pair_copy(pair_k, c, mine).start()
            return carry

        lax.fori_loop(0, CHUNKS, give, 0)

    @pl.when(is_source)
    def _():
        own_load.wait()

    def copy(link, k, c, device, span):
        piece = hid.at[k * CHUNKS + c, span]
        return pltpu.make_async_remote_copy(
            src_ref=piece,
            dst_ref=piece,
            send_sem=sent.at[link],
            recv_sem=recv.at[k, c],
            device_id=device,
            device_id_type=MESH,
        )

    def routes(k, c, dx, dy, szz, span):
        column = dx + dy == 0
        spot = ((y + dy) % 2) * 2 + (x + dx) % 2
        word = pick(c, [TALL[i] | VIA[i] << 8 | DEEP[i] << 20 for i in range(CHUNKS)])
        place = szz * 4 + spot
        tall = field(word, place, 1) == 1
        via = field(word, place + 8, 1)
        deep = field(word, place + 16, 1) == 1
        along = jnp.logical_or(
            jnp.logical_and(zz > szz, tall), jnp.logical_and(zz < szz, deep)
        )
        inplane = jnp.logical_not(along)
        via_x = jnp.logical_and(jnp.logical_and(dx == 0, dy == 1), via == 1)
        via_y = jnp.logical_and(jnp.logical_and(dx == 1, dy == 0), via == 0)
        go_up = jnp.logical_and(jnp.logical_or(column, tall), jnp.logical_and(zz >= szz, has_up))
        go_down = jnp.logical_and(jnp.logical_or(column, deep), jnp.logical_and(zz == 1, szz == 1))
        return (
            (go_up, copy(2, k, c, up_dev, span)),
            (go_down, copy(3, k, c, down_dev, span)),
            (jnp.logical_and(inplane, jnp.logical_or(column, via_x)), copy(0, k, c, x_dev, span)),
            (jnp.logical_and(inplane, jnp.logical_or(column, via_y)), copy(1, k, c, y_dev, span)),
        )

    def forward(k, c, dx, dy, szz, span):
        for condition, route in routes(k, c, dx, dy, szz, span):
            @pl.when(condition)
            def _():
                route.start()

    everything = pl.ds(0, rows)

    def item(q):
        r, i = q // 2, q % 2
        dx, dy = r % 2, r // 2
        first = jnp.where(zz >= 1, 1, 0)
        szz = first + i * (1 - 2 * first)
        src_z = szz + s * (DEPTH - 1 - 2 * szz)
        k = src_z * PLANE + ((y + dy) % 2) * 2 + (x + dx) % 2 - half_n * s
        return k, dx, dy, szz

    def send_own(c):
        @pl.when(jnp.logical_and(is_source, c < CHUNKS))
        def _():
            forward(own_k, c, 0, 0, zz, mine)
            pair_copy(own_k, c, theirs).wait_recv()
            forward(own_k, c, 0, 0, zz, theirs)

    def lead(c, carry):
        send_own(c)
        return carry

    lax.fori_loop(0, LEAD, lead, 0)

    pair_target.wait()

    @pl.when(jnp.logical_not(is_source))
    def _():
        for g in range(GROUPS):
            for ids, side in ((target, mine), (target_pair, theirs)):
                upright = jnp.broadcast_to(ids[:, g * rows : (g + 1) * rows], (LANES, rows)).T
                wanted[2 * g, side, :] = upright[:half]
                wanted[2 * g + 1, side, :] = upright[half:]

    load_w.wait()
    load_t.wait()

    def far_copy(g):
        return pltpu.make_async_remote_copy(
            src_ref=part.at[pl.ds(2 * g, 2)],
            dst_ref=far.at[pl.ds(2 * g, 2)],
            send_sem=far_sent.at[0],
            recv_sem=far_recv.at[g],
            device_id=pair_dev,
            device_id_type=MESH,
        )

    def stat_copy(g, core, d):
        return pltpu.make_async_remote_copy(
            src_ref=stats.at[g, 0],
            dst_ref=stats.at[g, d],
            send_sem=stat_sent.at[core],
            recv_sem=stat_recv.at[g],
            device_id=(core, v ^ d),
            device_id_type=MESH,
        )

    def sums(g):
        return (part[pl.ds(2 * g, 2)] + far[pl.ds(2 * g, 2)]).reshape(group_rows, 2 * width)

    def local_stats(g):
        far_copy(g).wait_recv()
        both = sums(g)
        logits, slope = both[:, :width], both[:, width:]
        top = jnp.max(logits, axis=1, keepdims=True)
        e = jnp.exp(logits - top)
        amount = jnp.sum(e, axis=1, keepdims=True)
        weighted = jnp.sum(e * slope, axis=1, keepdims=True)
        columns = lax.broadcasted_iota(jnp.int32, logits.shape, 1) + v * width
        ids = wanted[pl.ds(2 * g, 2)].reshape(group_rows, LANES)[:, 0:1]
        picked = jnp.sum(jnp.where(columns == ids, logits, 0.0), axis=1, keepdims=True)
        lane = lax.broadcasted_iota(jnp.int32, (group_rows, LANES), 1)
        packed = jnp.where(lane == 0, top, jnp.where(lane == 1, amount, jnp.where(lane == 2, weighted, picked)))
        stats[g, 0] = packed.T[:4]
        stat_copy(g, 1 - s, 0).start()

        def start(d, carry):
            stat_copy(g, 0, n - d).start()
            stat_copy(g, 1, n - d).start()
            return carry

        lax.fori_loop(1, n, start, 0)

    def finish(g):
        @pl.when(is_source)
        def _():
            far_copy(g).wait_recv()
            bulk(stats.at[g], stat_recv.at[g]).wait_recv()

        @pl.when(jnp.logical_not(is_source))
        def _():
            bulk(stats.at[g, pl.ds(1, n - 1)], stat_recv.at[g]).wait_recv()

        every = stats[g]
        tops = every[:, 0, :]
        row_top = jnp.max(tops, axis=0, keepdims=True)
        scale = jnp.exp(tops - row_top)
        totals = jnp.sum(scale * every[:, 1, :], axis=0, keepdims=True)
        tangent_sum = jnp.sum(scale * every[:, 2, :], axis=0, keepdims=True)
        picked = jnp.sum(every[:, 3, :], axis=0, keepdims=True)
        expect = tangent_sum / totals
        line = lax.broadcasted_iota(jnp.int32, (LANES, group_rows), 0)
        side = jnp.where(line == 0, row_top, jnp.where(line == 1, totals, expect)).T
        both = sums(g)
        value = jnp.exp(both[:, :width] - side[:, 0:1]) / side[:, 1:2] * (both[:, width:] - side[:, 2:3])
        term[pl.ds(2 * g, 2)] = value.astype(term.dtype).reshape(2, rows, width)
        loss = row_top + jnp.log(totals) - picked
        low, high = loss[:, :rows], loss[:, rows:]
        low = jnp.where(s == 0, low, pltpu.roll(low, half, 1))
        high = jnp.where(s == 1, high, pltpu.roll(high, half, 1))
        lane = lax.broadcasted_iota(jnp.int32, (1, rows), 1)
        loss_out[g] = jnp.where(lane < half, low, high)

    early = 2 * group_rows

    def first_product():
        right = term[pl.ds(0, 4)].reshape(early, width)

        def one(k, carry):
            total[k] = jnp.dot(flipped[k, :, pl.ds(0, early)], right, preferred_element_type=jnp.float32)
            return carry

        lax.fori_loop(0, half_n, one, 0, unroll=UNROLL)

    def second_product():
        right = term[pl.ds(4, 2)].reshape(group_rows, width)

        def one(k, carry):
            left = flipped[k, :, pl.ds(early, group_rows)]
            total[k] += jnp.dot(left, right, preferred_element_type=jnp.float32)
            return carry

        lax.fori_loop(0, half_n, one, 0, unroll=UNROLL)

    def ripe(done, act):
        @pl.when(jnp.logical_and(done >= 0, done % 2 == 1))
        def _():
            act(done // 2)

    def stages(done):
        @pl.when(jnp.logical_not(is_source))
        def _():
            ripe(done, local_stats)

            ripe(done - FINISH_LAG, finish)

    def step(t, carry):
        done = t - last_lag

        send_own(t + LEAD)
        def one(i, inner):
            q = field(order_word, i, 3)
            c = t - field(lag_word, q, 4)

            @pl.when(jnp.logical_and(c >= 0, c < CHUNKS))
            def _():
                k, dx, dy, szz = item(q)
                own = jnp.logical_and(dx + dy == 0, szz == zz)

                @pl.when(jnp.logical_not(own))
                def _():
                    copy(0, k, c, x_dev, everything).wait_recv()
                    forward(k, c, dx, dy, szz, everything)

                @pl.when(c % 2 == 1)
                def _():
                    two = hid[pl.ds(k * CHUNKS + c - 1, 2)].reshape(group_rows, hid.shape[2])
                    more = jnp.dot(two, both_w[k], preferred_element_type=jnp.float32)
                    part[pl.ds(c - 1, 2)] += more.reshape(2, rows, 2 * width)

                    @pl.when(c < CHUNKS - 2)
                    def _():
                        flipped[k, :, pl.ds(pl.multiple_of((c - 1) * rows, group_rows), group_rows)] = two.T

                    @pl.when(c >= CHUNKS - 2)
                    def _():
                        last[k] = two.T

            return inner

        lax.fori_loop(0, 8, one, 0)

        ripe(done, lambda g: far_copy(g).start())
        stages(done)
        return carry

    lax.fori_loop(0, CHUNKS + last_lag, step, 0)

    def owed(g, carry):
        finish(g)
        return carry

    lax.fori_loop(jnp.where(is_source, 0, FINISHED), GROUPS - 2, owed, 0)
    first_product()
    finish(GROUPS - 2)
    second_product()

    corners = [links_used(i // 4, i // 2 % 2, i % 2) for i in range(4 * DEPTH)]
    corner = zz * 4 + y * 2 + x
    for link in range(4):
        counts = [used[link] for used in corners]
        used = pick(corner, counts)
        for count in sorted(set(counts) - {0}):

            @pl.when(used == count)
            def _():
                bulk(hid.at[pl.ds(0, count)], sent.at[link]).wait_send()

    bulk(part, far_sent.at[0]).wait_send()

    @pl.when(jnp.logical_not(is_source))
    def _():
        bulk(staged, pair_sent.at[0]).wait_send()
        bulk(stats.at[:, pl.ds(1, n - 1)], stat_sent.at[s]).wait_send()
        bulk(stats, stat_sent.at[1 - s]).wait_send()

    finish(GROUPS - 1)


def product_kernel(total, last, term, loss_in, out, loss_out, rounded, sem):
    half_n = total.shape[0]
    right = term[pl.ds(CHUNKS - 2, 2)].reshape(last.shape[2], term.shape[2])

    def copy(k):
        return pltpu.make_async_copy(rounded.at[k], out.at[k], sem.at[k])

    def one(k, carry):
        rounded[k] = (total[k] + jnp.dot(last[k], right, preferred_element_type=jnp.float32)).astype(out.dtype)
        copy(k).start()
        return carry

    lax.fori_loop(0, half_n, one, 0, unroll=4)
    for g in range(GROUPS):
        loss_out[g * LANES : (g + 1) * LANES] = loss_in[g, 0]

    def settle(k, carry):
        copy(k).wait()
        return carry

    lax.fori_loop(0, half_n, settle, 0)


def relayed(n, hidden, weight, tangent, targets):
    half_n = n // 2
    tokens_own, shard = hidden.shape
    width = weight.shape[1]
    rows = 2 * tokens_own // CHUNKS
    blocks = (half_n, shard, width)
    hbm = pl.BlockSpec(memory_space=pltpu.HBM)
    vmem = pl.BlockSpec(memory_space=pltpu.VMEM)
    dma = pltpu.SemaphoreType.DMA
    total, last, term, loss = pl.pallas_call(
        functools.partial(gather_kernel, n),
        name="gather_logits",
        out_shape=(
            pltpu.VMEM(blocks, jnp.float32),
            pltpu.VMEM((half_n, shard, 2 * rows), hidden.dtype),
            pltpu.VMEM((CHUNKS, rows, width), jnp.bfloat16),
            pltpu.VMEM((GROUPS, 1, rows), jnp.float32),
        ),
        in_specs=[hbm, hbm, hbm, hbm],
        out_specs=(vmem, vmem, vmem, vmem),
        scratch_shapes=[
            pltpu.VMEM((half_n * CHUNKS, rows, shard), hidden.dtype),
            pltpu.VMEM((half_n, shard, (CHUNKS - 2) * rows), hidden.dtype),
            pltpu.VMEM((CHUNKS, rows // 2, shard), hidden.dtype),
            pltpu.VMEM((half_n, shard, 2 * width), weight.dtype),
            pltpu.VMEM((CHUNKS, rows, 2 * width), jnp.float32),
            pltpu.VMEM((CHUNKS, rows, 2 * width), jnp.float32),
            pltpu.VMEM((GROUPS, n, 4, 2 * rows), jnp.float32),
            pltpu.VMEM((1, tokens_own), jnp.int32),
            pltpu.VMEM((1, tokens_own), jnp.int32),
            pltpu.VMEM((CHUNKS, rows, LANES), jnp.int32),
            dma((half_n, CHUNKS)),
            dma((4,)),
            dma((CHUNKS,)),
            dma((1,)),
            dma((4,)),
            dma((1,)),
            dma((GROUPS,)),
            dma((2,)),
            dma((GROUPS,)),
            dma((2,)),
        ],
        compiler_params=pltpu.CompilerParams(
            collective_id=0, has_side_effects=True, vmem_limit_bytes=42 * 2**20
        ),
    )(
        pltpu.with_memory_space_constraint(hidden.reshape(CHUNKS, rows // 2, shard), pltpu.HBM),
        pltpu.with_memory_space_constraint(weight.reshape(blocks), pltpu.HBM),
        pltpu.with_memory_space_constraint(tangent.reshape(blocks), pltpu.HBM),
        pltpu.with_memory_space_constraint(targets.reshape(1, tokens_own), pltpu.HBM),
    )
    ggn, token_loss = pl.pallas_call(
        product_kernel,
        name="product",
        out_shape=(
            jax.ShapeDtypeStruct(blocks, jnp.bfloat16),
            jax.ShapeDtypeStruct((tokens_own,), jnp.float32),
        ),
        in_specs=[vmem, vmem, vmem, vmem],
        out_specs=(hbm, vmem),
        scratch_shapes=[pltpu.VMEM(blocks, jnp.bfloat16), dma((half_n,))],
        compiler_params=pltpu.CompilerParams(vmem_limit_bytes=20 * 2**20),
    )(total, last, term, loss)
    return ggn.reshape(weight.shape), token_loss


def partner(value, axis, stride):
    mask = 2**stride
    pairs = [(source, source ^ mask) for source in range(lax.axis_size(axis))]
    return lax.ppermute(value, axis, pairs)


def on_device(hidden, weight, tangent, targets):
    n = lax.axis_size("vocab")
    if n == PLANE * DEPTH and lax.axis_size("seq") == 2 and hidden.shape[0] == LANES * GROUPS and hidden.shape[1] % LANES == 0:
        return relayed(n, hidden, weight, tangent, targets)
    vocab_index = lax.axis_index("vocab")
    shard_width = weight.shape[1]
    half_width = weight.shape[0]
    whole = lax.all_gather(hidden, "vocab", axis=1, tiled=True)
    seq_index = lax.axis_index("seq")
    own_part = lax.dynamic_slice_in_dim(whole, seq_index * half_width, half_width, 1)
    far_part = lax.dynamic_slice_in_dim(whole, (1 - seq_index) * half_width, half_width, 1)
    received = partner(far_part, "seq", 0)
    leading = jnp.where(seq_index == 0, own_part, received)
    trailing = jnp.where(seq_index == 0, received, own_part)
    stacked = jnp.concatenate([leading, trailing], axis=0)
    partial_logits = jnp.dot(stacked, weight, preferred_element_type=jnp.float32)
    partial_tangent = jnp.dot(stacked, tangent, preferred_element_type=jnp.float32)
    logits, tangent_logits = (
        lax.psum_scatter(partial_logits, "seq", scatter_dimension=0, tiled=True),
        lax.psum_scatter(partial_tangent, "seq", scatter_dimension=0, tiled=True),
    )
    local_target = targets - vocab_index * shard_width
    columns_ids = jnp.arange(shard_width, dtype=jnp.int32)
    picked_local = jnp.sum(
        jnp.where(columns_ids[None, :] == local_target[:, None], logits, jnp.float32(0.0)), axis=1
    )
    local_top = jnp.max(logits, axis=1)
    row_top = lax.pmax(local_top, "vocab")
    exp_logits = jnp.exp(logits - row_top[:, None])
    totals, tangent_sum, picked = lax.psum(
        (jnp.sum(exp_logits, axis=1), jnp.sum(exp_logits * tangent_logits, axis=1), picked_local),
        "vocab",
    )
    expect = tangent_sum / totals
    token_loss = row_top + jnp.log(totals) - picked
    weight_term = (exp_logits / totals[:, None] * (tangent_logits - expect[:, None])).astype(
        jnp.bfloat16
    )
    far_term = partner(weight_term, "seq", 0)
    lead_term = jnp.where(seq_index == 0, weight_term, far_term)
    trail_term = jnp.where(seq_index == 0, far_term, weight_term)
    all_terms = jnp.concatenate([lead_term, trail_term], axis=0)
    ggn = jnp.einsum("td,tv->dv", stacked, all_terms, preferred_element_type=jnp.float32).astype(
        jnp.bfloat16
    )
    return (ggn, token_loss)


def solution(mesh):
    in_specs = (P("seq", "vocab"), P("seq", "vocab"), P("seq", "vocab"), P("seq"))
    out_specs = (P("seq", "vocab"), P("seq"))
    return jax.shard_map(
        on_device, mesh=mesh, in_specs=in_specs, out_specs=out_specs, check_vma=False
    )
```

```python
import functools

import jax
import jax.numpy as jnp
from jax import lax
from jax.experimental import pallas as pl
from jax.experimental.pallas import tpu as pltpu
from jax.sharding import PartitionSpec as P

MESH = pl.DeviceIdType.MESH
PLANE, DEPTH = 4, 4
CHUNKS = 8
GROUPS = CHUNKS // 2
LEAD = 3
LAGS = ((0, 0, 1, 3, 0, 3, 4, 5), (0, 0, 2, 2, 2, 3, 4, 5), (0, 0, 2, 3, 2, 3, 4, 5), (0, 0, 2, 2, 2, 2, 5, 5))
ORDERS = ((6, 4, 1, 2, 5, 7, 3, 0), (4, 1, 5, 6, 7, 2, 3, 0), (3, 5, 7, 0, 1, 4, 2, 6), (2, 0, 1, 4, 3, 6, 5, 7))
TALL = (205, 24, 2, 2, 3, 82, 5, 41)
DEEP = (1, 0, 0, 0, 2, 0, 0, 0)
VIA = (37, 238, 1, 253, 14, 92, 25, 192)
FINISH_LAG = 4
FINISHED = (CHUNKS - FINISH_LAG) // 2
LANES = 128
UNROLL = 8


def links_used(zz, y, x):
    used = [0, 0, 0, 0]
    for c in range(CHUNKS):
        for item in range(8):
            szz, dy, dx = item // 4, item // 2 % 2, item % 2
            spot = (y + dy) % 2 * 2 + (x + dx) % 2
            tall = TALL[c] >> (szz * 4 + spot) & 1
            deep = DEEP[c] >> spot & 1 and szz == 1
            via = VIA[c] >> (szz * 4 + spot) & 1
            column = dx + dy == 0
            inplane = not (zz > szz and tall or zz < szz and deep)
            used[0] += inplane and (column or (dx == 0 and dy == 1 and via == 1))
            used[1] += inplane and (column or (dx == 1 and dy == 0 and via == 0))
            used[2] += (column or tall) and zz >= szz and zz < DEPTH - 1
            used[3] += (column or deep) and zz == 1 and szz == 1
    return [int(u) for u in used]


def packed(values, bits):
    word = sum(value << (bits * i) for i, value in enumerate(values))
    return word - (word >> 31 << 32)


def pick(index, values):
    chosen = jnp.int32(values[0])
    for i, value in enumerate(values[1:]):
        chosen = jnp.where(index == i + 1, jnp.int32(value), chosen)
    return chosen


def field(word, index, bits):
    return (word >> (index * bits)) & (2**bits - 1)


def gather_kernel(
    n, hidden, weight, tangent, targets, total, last, term, loss_out,
    hid, flipped, staged, both_w, part, far, stats, target, target_pair, wanted,
    recv, sent, pair_recv, pair_sent, load_sem, far_sent, far_recv,
    stat_sent, stat_recv, target_sem,
):
    s = lax.axis_index("seq")
    v = lax.axis_index("vocab")
    half_n = n // 2
    rows = hid.shape[1]
    half = rows // 2
    group_rows = 2 * rows
    width = weight.shape[2]
    z, y, x = v // PLANE, (v // 2) % 2, v % 2
    zz = z + s * (DEPTH - 1 - 2 * z)
    up_step = PLANE * (1 - 2 * s)
    x_dev = (s, v + 1 - 2 * x)
    y_dev = (s, v + 2 - 4 * y)
    up_dev = (s, v + up_step)
    down_dev = (s, v - up_step)
    pair_dev = (1 - s, v)
    is_source = zz < DEPTH // 2
    has_up = zz < DEPTH - 1
    has_down = zz > 0
    along_count = has_up.astype(jnp.int32) + has_down.astype(jnp.int32)
    own_k = jnp.where(is_source, v - half_n * s, 0)
    pair_k = jnp.where(is_source, 0, v - half_n * (1 - s))
    lag_word = pick(zz, [packed(lags, 4) for lags in LAGS])
    order_word = pick(zz, [packed(order, 3) for order in ORDERS])
    last_lag = pick(zz, [max(lags) for lags in LAGS])

    mine = pl.ds(pl.multiple_of(s * half, half), half)
    theirs = pl.ds(pl.multiple_of((1 - s) * half, half), half)

    load_w = pltpu.make_async_copy(weight, both_w.at[:, :, pl.ds(0, width)], load_sem.at[0])
    load_t = pltpu.make_async_copy(tangent, both_w.at[:, :, pl.ds(width, width)], load_sem.at[1])
    load_target = pltpu.make_async_copy(targets, target, load_sem.at[2])

    own_load = pltpu.make_async_copy(hidden, hid.at[pl.ds(own_k * CHUNKS, CHUNKS), mine], load_sem.at[3])
    stage = pltpu.make_async_copy(hidden, staged, load_sem.at[3])

    def pair_copy(k, c, span):
        return pltpu.make_async_remote_copy(
            src_ref=staged.at[c],
            dst_ref=hid.at[k * CHUNKS + c, span],
            send_sem=pair_sent.at[0],
            recv_sem=pair_recv.at[c],
            device_id=pair_dev,
            device_id_type=MESH,
        )

    def bulk(ref, semaphore):
        return pltpu.make_async_remote_copy(
            src_ref=ref,
            dst_ref=ref,
            send_sem=semaphore,
            recv_sem=semaphore,
            device_id=pair_dev,
            device_id_type=MESH,
        )

    def greet(semaphore, device):
        pl.semaphore_signal(semaphore, inc=1, device_id=device, device_id_type=MESH)

    def greet_along(semaphore):
        @pl.when(has_up)
        def _():
            greet(semaphore, up_dev)

        @pl.when(has_down)
        def _():
            greet(semaphore, down_dev)

    barrier = pltpu.get_barrier_semaphore()
    greet(barrier, pair_dev)
    greet(barrier, x_dev)
    greet(barrier, y_dev)
    greet_along(barrier)

    @pl.when(is_source)
    def _():
        own_load.start()

    @pl.when(jnp.logical_not(is_source))
    def _():
        stage.start()

    load_target.start()
    load_w.start()
    load_t.start()

    def clear(i, carry):
        part[i] = jnp.zeros(part.shape[1:], jnp.float32)
        return carry

    lax.fori_loop(0, CHUNKS, clear, 0)
    load_target.wait()
    pl.semaphore_wait(barrier, 3 + along_count)
    pair_target = pltpu.make_async_remote_copy(
        src_ref=target,
        dst_ref=target_pair,
        send_sem=target_sem.at[0],
        recv_sem=target_sem.at[1],
        device_id=pair_dev,
        device_id_type=MESH,
    )
    pair_target.start()

    @pl.when(jnp.logical_not(is_source))
    def _():
        stage.wait()

        def give(c, carry):
            pair_copy(pair_k, c, mine).start()
            return carry

        lax.fori_loop(0, CHUNKS, give, 0)

    @pl.when(is_source)
    def _():
        own_load.wait()

    def copy(link, k, c, device, span):
        piece = hid.at[k * CHUNKS + c, span]
        return pltpu.make_async_remote_copy(
            src_ref=piece,
            dst_ref=piece,
            send_sem=sent.at[link],
            recv_sem=recv.at[k, c],
            device_id=device,
            device_id_type=MESH,
        )

    def routes(k, c, dx, dy, szz, span):
        column = dx + dy == 0
        spot = ((y + dy) % 2) * 2 + (x + dx) % 2
        word = pick(c, [TALL[i] | VIA[i] << 8 | DEEP[i] << 20 for i in range(CHUNKS)])
        place = szz * 4 + spot
        tall = field(word, place, 1) == 1
        via = field(word, place + 8, 1)
        deep = field(word, place + 16, 1) == 1
        along = jnp.logical_or(
            jnp.logical_and(zz > szz, tall), jnp.logical_and(zz < szz, deep)
        )
        inplane = jnp.logical_not(along)
        via_x = jnp.logical_and(jnp.logical_and(dx == 0, dy == 1), via == 1)
        via_y = jnp.logical_and(jnp.logical_and(dx == 1, dy == 0), via == 0)
        go_up = jnp.logical_and(jnp.logical_or(column, tall), jnp.logical_and(zz >= szz, has_up))
        go_down = jnp.logical_and(jnp.logical_or(column, deep), jnp.logical_and(zz == 1, szz == 1))
        return (
            (go_up, copy(2, k, c, up_dev, span)),
            (go_down, copy(3, k, c, down_dev, span)),
            (jnp.logical_and(inplane, jnp.logical_or(column, via_x)), copy(0, k, c, x_dev, span)),
            (jnp.logical_and(inplane, jnp.logical_or(column, via_y)), copy(1, k, c, y_dev, span)),
        )

    def forward(k, c, dx, dy, szz, span):
        for condition, route in routes(k, c, dx, dy, szz, span):
            @pl.when(condition)
            def _():
                route.start()

    everything = pl.ds(0, rows)

    def item(q):
        r, i = q // 2, q % 2
        dx, dy = r % 2, r // 2
        first = jnp.where(zz >= 1, 1, 0)
        szz = first + i * (1 - 2 * first)
        src_z = szz + s * (DEPTH - 1 - 2 * szz)
        k = src_z * PLANE + ((y + dy) % 2) * 2 + (x + dx) % 2 - half_n * s
        return k, dx, dy, szz

    def send_own(c):
        @pl.when(jnp.logical_and(is_source, c < CHUNKS))
        def _():
            forward(own_k, c, 0, 0, zz, mine)
            pair_copy(own_k, c, theirs).wait_recv()
            forward(own_k, c, 0, 0, zz, theirs)

    def lead(c, carry):
        send_own(c)
        return carry

    lax.fori_loop(0, LEAD, lead, 0)

    pair_target.wait()

    @pl.when(jnp.logical_not(is_source))
    def _():
        for g in range(GROUPS):
            for ids, side in ((target, mine), (target_pair, theirs)):
                upright = jnp.broadcast_to(ids[:, g * rows : (g + 1) * rows], (LANES, rows)).T
                wanted[2 * g, side, :] = upright[:half]
                wanted[2 * g + 1, side, :] = upright[half:]

    load_w.wait()
    load_t.wait()

    def far_copy(g):
        return pltpu.make_async_remote_copy(
            src_ref=part.at[pl.ds(2 * g, 2)],
            dst_ref=far.at[pl.ds(2 * g, 2)],
            send_sem=far_sent.at[0],
            recv_sem=far_recv.at[g],
            device_id=pair_dev,
            device_id_type=MESH,
        )

    def stat_copy(g, core, d):
        return pltpu.make_async_remote_copy(
            src_ref=stats.at[g, 0],
            dst_ref=stats.at[g, d],
            send_sem=stat_sent.at[core],
            recv_sem=stat_recv.at[g],
            device_id=(core, v ^ d),
            device_id_type=MESH,
        )

    def sums(g):
        return (part[pl.ds(2 * g, 2)] + far[pl.ds(2 * g, 2)]).reshape(group_rows, 2 * width)

    def local_stats(g):
        far_copy(g).wait_recv()
        both = sums(g)
        logits, slope = both[:, :width], both[:, width:]
        top = jnp.max(logits, axis=1, keepdims=True)
        e = jnp.exp(logits - top)
        amount = jnp.sum(e, axis=1, keepdims=True)
        weighted = jnp.sum(e * slope, axis=1, keepdims=True)
        columns = lax.broadcasted_iota(jnp.int32, logits.shape, 1) + v * width
        ids = wanted[pl.ds(2 * g, 2)].reshape(group_rows, LANES)[:, 0:1]
        picked = jnp.sum(jnp.where(columns == ids, logits, 0.0), axis=1, keepdims=True)
        lane = lax.broadcasted_iota(jnp.int32, (group_rows, LANES), 1)
        packed = jnp.where(lane == 0, top, jnp.where(lane == 1, amount, jnp.where(lane == 2, weighted, picked)))
        stats[g, 0] = packed.T[:4]
        stat_copy(g, 1 - s, 0).start()

        def start(d, carry):
            stat_copy(g, 0, n - d).start()
            stat_copy(g, 1, n - d).start()
            return carry

        lax.fori_loop(1, n, start, 0, unroll=5)

    def finish(g):
        @pl.when(is_source)
        def _():
            far_copy(g).wait_recv()
            bulk(stats.at[g], stat_recv.at[g]).wait_recv()

        @pl.when(jnp.logical_not(is_source))
        def _():
            bulk(stats.at[g, pl.ds(1, n - 1)], stat_recv.at[g]).wait_recv()

        every = stats[g]
        tops = every[:, 0, :]
        row_top = jnp.max(tops, axis=0, keepdims=True)
        scale = jnp.exp(tops - row_top)
        totals = jnp.sum(scale * every[:, 1, :], axis=0, keepdims=True)
        tangent_sum = jnp.sum(scale * every[:, 2, :], axis=0, keepdims=True)
        picked = jnp.sum(every[:, 3, :], axis=0, keepdims=True)
        expect = tangent_sum / totals
        line = lax.broadcasted_iota(jnp.int32, (LANES, group_rows), 0)
        side = jnp.where(line == 0, row_top, jnp.where(line == 1, totals, expect)).T
        both = sums(g)
        value = jnp.exp(both[:, :width] - side[:, 0:1]) / side[:, 1:2] * (both[:, width:] - side[:, 2:3])
        term[pl.ds(2 * g, 2)] = value.astype(term.dtype).reshape(2, rows, width)
        loss = row_top + jnp.log(totals) - picked
        low, high = loss[:, :rows], loss[:, rows:]
        low = jnp.where(s == 0, low, pltpu.roll(low, half, 1))
        high = jnp.where(s == 1, high, pltpu.roll(high, half, 1))
        lane = lax.broadcasted_iota(jnp.int32, (1, rows), 1)
        loss_out[g] = jnp.where(lane < half, low, high)

    early = 2 * group_rows

    def first_product():
        right = term[pl.ds(0, 4)].reshape(early, width)

        def one(k, carry):
            total[k] = jnp.dot(flipped[k, :, pl.ds(0, early)], right, preferred_element_type=jnp.float32)
            return carry

        lax.fori_loop(0, half_n, one, 0, unroll=UNROLL)

    def second_product():
        right = term[pl.ds(4, 2)].reshape(group_rows, width)

        def one(k, carry):
            left = flipped[k, :, pl.ds(early, group_rows)]
            total[k] += jnp.dot(left, right, preferred_element_type=jnp.float32)
            return carry

        lax.fori_loop(0, half_n, one, 0, unroll=UNROLL)

    def ripe(done, act):
        @pl.when(jnp.logical_and(done >= 0, done % 2 == 1))
        def _():
            act(done // 2)

    def stages(done):
        @pl.when(jnp.logical_not(is_source))
        def _():
            ripe(done, local_stats)

            ripe(done - FINISH_LAG, finish)

    def step(t, carry):
        done = t - last_lag

        send_own(t + LEAD)
        def one(i, inner):
            q = field(order_word, i, 3)
            c = t - field(lag_word, q, 4)

            @pl.when(jnp.logical_and(c >= 0, c < CHUNKS))
            def _():
                k, dx, dy, szz = item(q)
                own = jnp.logical_and(dx + dy == 0, szz == zz)

                @pl.when(jnp.logical_not(own))
                def _():
                    copy(0, k, c, x_dev, everything).wait_recv()
                    forward(k, c, dx, dy, szz, everything)

                @pl.when(c % 2 == 1)
                def _():
                    two = hid[pl.ds(k * CHUNKS + c - 1, 2)].reshape(group_rows, hid.shape[2])
                    more = jnp.dot(two, both_w[k], preferred_element_type=jnp.float32)
                    part[pl.ds(c - 1, 2)] += more.reshape(2, rows, 2 * width)

                    @pl.when(c < CHUNKS - 2)
                    def _():
                        flipped[k, :, pl.ds(pl.multiple_of((c - 1) * rows, group_rows), group_rows)] = two.T

                    @pl.when(c >= CHUNKS - 2)
                    def _():
                        last[k] = two.T

            return inner

        lax.fori_loop(0, 8, one, 0)

        ripe(done, lambda g: far_copy(g).start())
        stages(done)
        return carry

    lax.fori_loop(0, CHUNKS + last_lag, step, 0)

    def owed(g, carry):
        finish(g)
        return carry

    lax.fori_loop(jnp.where(is_source, 0, FINISHED), GROUPS - 2, owed, 0)
    first_product()
    finish(GROUPS - 2)
    second_product()

    corners = [links_used(i // 4, i // 2 % 2, i % 2) for i in range(4 * DEPTH)]
    corner = zz * 4 + y * 2 + x
    for link in range(4):
        counts = [used[link] for used in corners]
        used = pick(corner, counts)
        for count in sorted(set(counts) - {0}):

            @pl.when(used == count)
            def _():
                bulk(hid.at[pl.ds(0, count)], sent.at[link]).wait_send()

    bulk(part, far_sent.at[0]).wait_send()

    @pl.when(jnp.logical_not(is_source))
    def _():
        bulk(staged, pair_sent.at[0]).wait_send()
        bulk(stats.at[:, pl.ds(1, n - 1)], stat_sent.at[s]).wait_send()
        bulk(stats, stat_sent.at[1 - s]).wait_send()

    finish(GROUPS - 1)


def product_kernel(total, last, term, loss_in, out, loss_out, rounded, sem):
    half_n = total.shape[0]
    right = term[pl.ds(CHUNKS - 2, 2)].reshape(last.shape[2], term.shape[2])

    def copy(k):
        return pltpu.make_async_copy(rounded.at[k], out.at[k], sem.at[k])

    def one(k, carry):
        rounded[k] = (total[k] + jnp.dot(last[k], right, preferred_element_type=jnp.float32)).astype(out.dtype)
        copy(k).start()
        return carry

    lax.fori_loop(0, half_n, one, 0, unroll=8)
    for g in range(GROUPS):
        loss_out[g * LANES : (g + 1) * LANES] = loss_in[g, 0]

    def settle(k, carry):
        copy(k).wait()
        return carry

    lax.fori_loop(0, half_n, settle, 0)


def relayed(n, hidden, weight, tangent, targets):
    half_n = n // 2
    tokens_own, shard = hidden.shape
    width = weight.shape[1]
    rows = 2 * tokens_own // CHUNKS
    blocks = (half_n, shard, width)
    hbm = pl.BlockSpec(memory_space=pltpu.HBM)
    vmem = pl.BlockSpec(memory_space=pltpu.VMEM)
    dma = pltpu.SemaphoreType.DMA
    total, last, term, loss = pl.pallas_call(
        functools.partial(gather_kernel, n),
        name="gather_logits",
        out_shape=(
            pltpu.VMEM(blocks, jnp.float32),
            pltpu.VMEM((half_n, shard, 2 * rows), hidden.dtype),
            pltpu.VMEM((CHUNKS, rows, width), jnp.bfloat16),
            pltpu.VMEM((GROUPS, 1, rows), jnp.float32),
        ),
        in_specs=[hbm, hbm, hbm, hbm],
        out_specs=(vmem, vmem, vmem, vmem),
        scratch_shapes=[
            pltpu.VMEM((half_n * CHUNKS, rows, shard), hidden.dtype),
            pltpu.VMEM((half_n, shard, (CHUNKS - 2) * rows), hidden.dtype),
            pltpu.VMEM((CHUNKS, rows // 2, shard), hidden.dtype),
            pltpu.VMEM((half_n, shard, 2 * width), weight.dtype),
            pltpu.VMEM((CHUNKS, rows, 2 * width), jnp.float32),
            pltpu.VMEM((CHUNKS, rows, 2 * width), jnp.float32),
            pltpu.VMEM((GROUPS, n, 4, 2 * rows), jnp.float32),
            pltpu.VMEM((1, tokens_own), jnp.int32),
            pltpu.VMEM((1, tokens_own), jnp.int32),
            pltpu.VMEM((CHUNKS, rows, LANES), jnp.int32),
            dma((half_n, CHUNKS)),
            dma((4,)),
            dma((CHUNKS,)),
            dma((1,)),
            dma((4,)),
            dma((1,)),
            dma((GROUPS,)),
            dma((2,)),
            dma((GROUPS,)),
            dma((2,)),
        ],
        compiler_params=pltpu.CompilerParams(
            collective_id=0, has_side_effects=True, vmem_limit_bytes=42 * 2**20
        ),
    )(
        pltpu.with_memory_space_constraint(hidden.reshape(CHUNKS, rows // 2, shard), pltpu.HBM),
        pltpu.with_memory_space_constraint(weight.reshape(blocks), pltpu.HBM),
        pltpu.with_memory_space_constraint(tangent.reshape(blocks), pltpu.HBM),
        pltpu.with_memory_space_constraint(targets.reshape(1, tokens_own), pltpu.HBM),
    )
    ggn, token_loss = pl.pallas_call(
        product_kernel,
        name="product",
        out_shape=(
            jax.ShapeDtypeStruct(blocks, jnp.bfloat16),
            jax.ShapeDtypeStruct((tokens_own,), jnp.float32),
        ),
        in_specs=[vmem, vmem, vmem, vmem],
        out_specs=(hbm, vmem),
        scratch_shapes=[pltpu.VMEM(blocks, jnp.bfloat16), dma((half_n,))],
        compiler_params=pltpu.CompilerParams(vmem_limit_bytes=20 * 2**20),
    )(total, last, term, loss)
    return ggn.reshape(weight.shape), token_loss


def partner(value, axis, stride):
    mask = 2**stride
    pairs = [(source, source ^ mask) for source in range(lax.axis_size(axis))]
    return lax.ppermute(value, axis, pairs)


def on_device(hidden, weight, tangent, targets):
    n = lax.axis_size("vocab")
    if n == PLANE * DEPTH and lax.axis_size("seq") == 2 and hidden.shape[0] == LANES * GROUPS and hidden.shape[1] % LANES == 0:
        return relayed(n, hidden, weight, tangent, targets)
    vocab_index = lax.axis_index("vocab")
    shard_width = weight.shape[1]
    half_width = weight.shape[0]
    whole = lax.all_gather(hidden, "vocab", axis=1, tiled=True)
    seq_index = lax.axis_index("seq")
    own_part = lax.dynamic_slice_in_dim(whole, seq_index * half_width, half_width, 1)
    far_part = lax.dynamic_slice_in_dim(whole, (1 - seq_index) * half_width, half_width, 1)
    received = partner(far_part, "seq", 0)
    leading = jnp.where(seq_index == 0, own_part, received)
    trailing = jnp.where(seq_index == 0, received, own_part)
    stacked = jnp.concatenate([leading, trailing], axis=0)
    partial_logits = jnp.dot(stacked, weight, preferred_element_type=jnp.float32)
    partial_tangent = jnp.dot(stacked, tangent, preferred_element_type=jnp.float32)
    logits, tangent_logits = (
        lax.psum_scatter(partial_logits, "seq", scatter_dimension=0, tiled=True),
        lax.psum_scatter(partial_tangent, "seq", scatter_dimension=0, tiled=True),
    )
    local_target = targets - vocab_index * shard_width
    columns_ids = jnp.arange(shard_width, dtype=jnp.int32)
    picked_local = jnp.sum(
        jnp.where(columns_ids[None, :] == local_target[:, None], logits, jnp.float32(0.0)), axis=1
    )
    local_top = jnp.max(logits, axis=1)
    row_top = lax.pmax(local_top, "vocab")
    exp_logits = jnp.exp(logits - row_top[:, None])
    totals, tangent_sum, picked = lax.psum(
        (jnp.sum(exp_logits, axis=1), jnp.sum(exp_logits * tangent_logits, axis=1), picked_local),
        "vocab",
    )
    expect = tangent_sum / totals
    token_loss = row_top + jnp.log(totals) - picked
    weight_term = (exp_logits / totals[:, None] * (tangent_logits - expect[:, None])).astype(
        jnp.bfloat16
    )
    far_term = partner(weight_term, "seq", 0)
    lead_term = jnp.where(seq_index == 0, weight_term, far_term)
    trail_term = jnp.where(seq_index == 0, far_term, weight_term)
    all_terms = jnp.concatenate([lead_term, trail_term], axis=0)
    ggn = jnp.einsum("td,tv->dv", stacked, all_terms, preferred_element_type=jnp.float32).astype(
        jnp.bfloat16
    )
    return (ggn, token_loss)


def solution(mesh):
    in_specs = (P("seq", "vocab"), P("seq", "vocab"), P("seq", "vocab"), P("seq"))
    out_specs = (P("seq", "vocab"), P("seq"))
    return jax.shard_map(
        on_device, mesh=mesh, in_specs=in_specs, out_specs=out_specs, check_vma=False
    )
```
